256 devices in a mesh: col: 4 (over x), row: 64 (over z, y, core).
Axes of the slice: x: 4, y: 4, z: 8, core: 2. Of those that a mesh axis runs over, the one named last changes fastest.
Arguments:
- inter_mask: int32 [65536, 4096], P('row', 'col')
- emb_user: bfloat16 [65536, 64], P(('row', 'col'))
- emb_item: bfloat16 [4096, 64], P(('col', 'row'))
- triples: int32 [1024, 3], replicated
Outputs:
- output 1: bfloat16 [65536, 64], P(('row', 'col'))
- output 2: bfloat16 [4096, 64], P(('col', 'row'))
- output 3: float32 [1024], replicated
All inputs are finite; a program needn't handle non-finite values.
Results may differ from the reference program's by a relative error of at most 0.00555861.
Values are sent between devices in bfloat16 or wider.
A program may use at most 768 MiB of HBM per device.

```python
import jax
import jax.numpy as jnp
from jax import lax

EMB = 64
LAYERS = 3
USERS = 65536
ITEMS = 4096
BATCH = 1024
ACT_MAX = 8
DENS_DIV = 256


def draw_mask(base_key):
    key_user, key_item, key_edge = jax.random.split(base_key, 3)
    user_act = jax.random.randint(key_user, (USERS, 1), 1, ACT_MAX + 1)
    item_pop = jax.random.randint(key_item, (1, ITEMS), 1, ACT_MAX + 1)
    edge_draw = jax.random.randint(key_edge, (USERS, ITEMS), 0, DENS_DIV)
    return (edge_draw < user_act * item_pop).astype(jnp.int32)


def draw_triples(base_key):
    key_user, key_pos, key_neg = jax.random.split(base_key, 3)
    user_ids = jax.random.randint(key_user, (BATCH,), 0, USERS)
    pos_ids = jax.random.randint(key_pos, (BATCH,), 0, ITEMS)
    neg_ids = jax.random.randint(key_neg, (BATCH,), 0, ITEMS)
    return jnp.stack([user_ids, pos_ids, neg_ids], axis=1).astype(jnp.int32)


def setup_inputs(seed: int = 0) -> dict:
    sub_keys = jax.random.split(jax.random.key(seed), 8)
    user_mean = jax.random.normal(sub_keys[1], (1, EMB), jnp.float32)
    user_noise = jax.random.normal(sub_keys[2], (USERS, EMB), jnp.float32)
    user_walk = jnp.cumsum(jax.random.normal(sub_keys[6], (USERS, EMB), jnp.float32), axis=0) * (USERS ** -0.5)
    item_mean = jax.random.normal(sub_keys[3], (1, EMB), jnp.float32)
    item_noise = jax.random.normal(sub_keys[4], (ITEMS, EMB), jnp.float32)
    item_walk = jnp.cumsum(jax.random.normal(sub_keys[7], (ITEMS, EMB), jnp.float32), axis=0) * (ITEMS ** -0.5)
    return {
        "inter_mask": draw_mask(sub_keys[0]),
        "emb_user": (0.5 * (user_mean + user_noise + user_walk)).astype(jnp.bfloat16),
        "emb_item": (0.5 * (item_mean + item_noise + item_walk)).astype(jnp.bfloat16),
        "triples": draw_triples(sub_keys[5]),
    }


def reference(inter_mask, emb_user, emb_item, triples):
    deg_user = jnp.maximum(jnp.sum(inter_mask, axis=1), 1).astype(jnp.float32)
    deg_item = jnp.maximum(jnp.sum(inter_mask, axis=0), 1).astype(jnp.float32)
    adj_norm = (inter_mask.astype(jnp.float32) * lax.rsqrt(deg_user)[:, None] * lax.rsqrt(deg_item)[None, :]).astype(jnp.bfloat16)

    def layer_step(carry, unused):
        cur_user, cur_item, total_user, total_item = carry
        next_user = jnp.dot(adj_norm, cur_item, preferred_element_type=jnp.float32).astype(jnp.bfloat16)
        next_item = jnp.dot(adj_norm.T, cur_user, preferred_element_type=jnp.float32).astype(jnp.bfloat16)
        new_carry = (next_user, next_item, total_user + next_user.astype(jnp.float32), total_item + next_item.astype(jnp.float32))
        return new_carry, None

    start_carry = (emb_user, emb_item, emb_user.astype(jnp.float32), emb_item.astype(jnp.float32))
    final_carry, unused_out = lax.scan(layer_step, start_carry, None, length=LAYERS)
    out_user = (final_carry[2] / (LAYERS + 1)).astype(jnp.bfloat16)
    out_item = (final_carry[3] / (LAYERS + 1)).astype(jnp.bfloat16)
    vec_user = out_user[triples[:, 0]].astype(jnp.float32)
    vec_pos = out_item[triples[:, 1]].astype(jnp.float32)
    vec_neg = out_item[triples[:, 2]].astype(jnp.float32)
    margin = jnp.sum(vec_user * vec_pos, axis=1) - jnp.sum(vec_user * vec_neg, axis=1)
    bpr_loss = jax.nn.softplus(-margin)
    return out_user, out_item, bpr_loss
```

```python
import functools

import jax
import jax.numpy as jnp
from jax import lax
from jax.experimental import pallas as pl
from jax.experimental.pallas import tpu as pltpu
from jax.sharding import PartitionSpec as P

LAYERS = 3
LANES = 128
F32 = jnp.float32
BF16 = jnp.bfloat16
NT = (((1,), (1,)), ((), ()))
NN = (((1,), (0,)), ((), ()))

STAGES = (
    ("deg_user", "x"), ("deg_item_a", "yc"), ("deg_item_b", "z"),
    ("emb_user", "x"), ("emb_item_a", "yc"), ("emb_item_b", "z"),
    ("urs1", "x"), ("urs2", "x"), ("urs3", "x"),
    ("uag1", "x"), ("uag2", "x"), ("uag3", "x"),
    ("irs1", "yc"), ("irs2", "yc"), ("irs3", "yc"),
    ("izz1", "z"), ("izz2", "z"), ("izz3", "z"),
    ("iag1", "yc"), ("iag2", "yc"), ("iag3", "yc"),
    ("loss_x", "x"), ("loss_yc", "yc"), ("loss_z", "z"),
)
SID = {name: idx for idx, (name, _) in enumerate(STAGES)}
GROUP = dict(STAGES)
OFFSETS = {"x": (2, 1, 3), "yc": (4, 5, 3, 2, 6, 7, 1), "z": (4, 3, 5, 2, 6, 1, 7)}
SIZE = {"x": 4, "yc": 8, "z": 8}


def mm(lhs, rhs, dims):
    return lax.dot_general(lhs, rhs, dims, preferred_element_type=F32)


def eye(rows, cols):
    row_id = lax.broadcasted_iota(jnp.int32, (rows, cols), 0)
    col_id = lax.broadcasted_iota(jnp.int32, (rows, cols), 1)
    return jnp.where(row_id == col_id, 1.0, 0.0).astype(BF16)


def kernel(axis_names, mask_hbm, user_ref, item_ref, trip_ref,
           out_user_ref, out_item_ref, loss_ref,
           mask_v, mask_b, adj, hot_user, hot_item, row_part, su_col, si_row, row_t,
           small_src, item_tr, user_src, part_user, own_user, part_item, own_item, marg,
           deg_user_s, deg_item_a, deg_item_b, emb_user_s, emb_item_a, emb_item_b,
           urs1, urs2, urs3, uag1, uag2, uag3,
           irs1, irs2, irs3, izz1, izz2, izz3, iag1, iag2, iag3,
           loss_x, loss_yc, loss_z,
           load_sem, send_sem, recv_sem):
    slots = {"deg_user": deg_user_s, "deg_item_a": deg_item_a, "deg_item_b": deg_item_b,
             "emb_user": emb_user_s, "emb_item_a": emb_item_a, "emb_item_b": emb_item_b,
             "urs1": urs1, "urs2": urs2, "urs3": urs3, "uag1": uag1, "uag2": uag2, "uag3": uag3,
             "irs1": irs1, "irs2": irs2, "irs3": irs3, "izz1": izz1, "izz2": izz2, "izz3": izz3,
             "iag1": iag1, "iag2": iag2, "iag3": iag3,
             "loss_x": loss_x, "loss_yc": loss_yc, "loss_z": loss_z}
    row = lax.axis_index("row")
    col = lax.axis_index("col")
    zed = row // 8
    pos = row % 8
    here = {"x": col, "yc": pos, "z": zed}

    def device(group, idx):
        coord = {"col": col, "row": row}
        if group == "x":
            coord["col"] = idx
        elif group == "yc":
            coord["row"] = zed * 8 + idx
        else:
            coord["row"] = idx * 8 + pos
        return tuple(coord[name] for name in axis_names)

    def peers(group):
        return [(here[group] + off) % SIZE[group] for off in OFFSETS[group]]

    def send(name, src, idx):
        group = GROUP[name]
        pltpu.make_async_remote_copy(
            src_ref=src, dst_ref=slots[name].at[here[group]],
            send_sem=send_sem.at[SID[name]], recv_sem=recv_sem.at[SID[name]],
            device_id=device(group, idx), device_id_type=pl.DeviceIdType.MESH).start()

    def send_all(name, src):
        for idx in peers(GROUP[name]):
            send(name, src, idx)

    def whole(name):
        group = GROUP[name]
        part = slots[name].at[pl.ds(0, SIZE[group] - 1)]
        return pltpu.make_async_remote_copy(
            src_ref=part, dst_ref=part,
            send_sem=send_sem.at[SID[name]], recv_sem=recv_sem.at[SID[name]],
            device_id=device(group, (here[group] + 1) % SIZE[group]),
            device_id_type=pl.DeviceIdType.MESH)

    def arrive(name):
        whole(name).wait_recv()

    def total(name):
        buf = slots[name]
        acc = buf[0]
        for idx in range(1, SIZE[GROUP[name]]):
            acc = acc + buf[idx]
        return acc

    def panel(name):
        buf = slots[name]
        return jnp.concatenate([buf[idx] for idx in range(SIZE[GROUP[name]])], axis=1)

    barrier = pltpu.get_barrier_semaphore()
    n_peers = 0
    for group in ("z", "yc", "x"):
        for idx in peers(group):
            pl.semaphore_signal(barrier, inc=1, device_id=device(group, idx),
                                device_id_type=pl.DeviceIdType.MESH)
            n_peers += 1
    loads = []
    for q in range(4):
        cp = pltpu.make_async_copy(mask_hbm.at[pl.ds(q * 256, 256)], mask_v.at[pl.ds(q * 256, 256)], load_sem.at[q])
        cp.start()
        loads.append(cp)
    eye64 = eye(64, 64)
    user_t = mm(eye64, user_ref[...], NT).astype(BF16)
    user_src[0] = user_t
    emb_user_s[col] = user_t
    emb_item_a[pos] = item_ref[...]
    pl.semaphore_wait(barrier, n_peers)
    send_all("emb_item_a", item_ref)
    send_all("emb_user", user_src.at[0])

    def degree_rows(blk, acc):
        base = pl.multiple_of(blk * 32, 32)
        m = mask_v[pl.ds(base, 32), :].astype(F32)
        mask_b[pl.ds(base, 32), :] = m.astype(BF16)
        part = m[:, 0:LANES]
        for k in range(1, 8):
            part = part + m[:, k * LANES:(k + 1) * LANES]
        row_part[pl.ds(base, 32), :] = part.astype(BF16)
        return acc + ((m[0:8] + m[8:16]) + (m[16:24] + m[24:32]))

    acc = jnp.zeros((8, 1024), F32)
    for q in range(4):
        loads[q].wait()
        acc = lax.fori_loop(q * 8, (q + 1) * 8, degree_rows, acc)
    col_sum = jnp.sum(acc, axis=0, keepdims=True)
    for k in range(8):
        small_src[0, k:k + 1, :] = col_sum[:, k * LANES:(k + 1) * LANES]
    deg_item_a[pos] = small_src[0]
    send_all("deg_item_a", small_src.at[0])
    row_sum = mm(jnp.ones((8, LANES), BF16), row_part[...], NT)
    for k in range(8):
        small_src[1, k:k + 1, :] = row_sum[0:1, k * LANES:(k + 1) * LANES]
    deg_user_s[col] = small_src[1]
    send_all("deg_user", small_src.at[1])

    def one_hot(blk, carry):
        base = pl.multiple_of(blk * 16, 16)
        trip = trip_ref[pl.ds(base, 16), :]
        lane = lax.broadcasted_iota(jnp.int32, (16, 1024), 1)
        hit = lambda ids: jnp.where(ids == lane, 1.0, 0.0)
        hot_user[pl.ds(base, 16), :] = hit(trip[:, 0:1] - row * 1024).astype(BF16)
        hot_item[pl.ds(base, 16), :] = (hit(trip[:, 1:2] - col * 1024) - hit(trip[:, 2:3] - col * 1024)).astype(BF16)
        return carry

    arrive("emb_item_a")
    gathered = jnp.concatenate([emb_item_a[k] for k in range(8)], axis=0)
    item_t = mm(eye64, gathered, NT).astype(BF16)
    item_tr[...] = item_t
    emb_item_b[zed] = item_t
    send_all("emb_item_b", item_tr)
    lax.fori_loop(0, 32, one_hot, 0)
    arrive("deg_item_a")
    deg_sum = total("deg_item_a")
    small_src[2] = deg_sum
    deg_item_b[zed] = deg_sum
    send_all("deg_item_b", small_src.at[2])
    lax.fori_loop(32, 64, one_hot, 0)
    arrive("deg_user")
    scale_user = lax.rsqrt(jnp.maximum(total("deg_user"), 1.0))
    for k in range(8):
        su_col[pl.ds(k * LANES, LANES), :] = jnp.transpose(jnp.broadcast_to(scale_user[k:k + 1, :], (LANES, LANES)))
    arrive("emb_user")
    arrive("emb_item_b")
    arrive("deg_item_b")
    scale_item = lax.rsqrt(jnp.maximum(total("deg_item_b"), 1.0))
    for k in range(8):
        si_row[:, k * LANES:(k + 1) * LANES] = jnp.broadcast_to(scale_item[k:k + 1, :], (8, LANES))

    def build(blk, carry):
        base = pl.multiple_of(blk * 16, 16)
        m = mask_b[pl.ds(base, 16), :].astype(F32)
        su = su_col[pl.ds(base, 16), :]
        for k in range(8):
            si = si_row[0:8, k * LANES:(k + 1) * LANES]
            si2 = jnp.concatenate([si, si], axis=0)
            adj[pl.ds(base, 16), k * LANES:(k + 1) * LANES] = ((m[:, k * LANES:(k + 1) * LANES] * su) * si2).astype(BF16)
        return carry

    lax.fori_loop(0, 64, build, 0)

    yy = pos // 2

    def item_products(layer, user_panel):
        name = f"irs{layer}"
        buf = part_item.at[layer - 1]
        for off in (2, 1, 3, 0):
            other = (yy + off) % 4
            cols = pl.ds(pl.multiple_of(other * 256, 256), 256)
            res = mm(user_panel, adj[:, cols], NN)
            buf[other * 2] = res[:, 0:LANES]
            buf[other * 2 + 1] = res[:, LANES:2 * LANES]
            if off:
                send(name, buf.at[other * 2], other * 2)
                send(name, buf.at[other * 2 + 1], other * 2 + 1)
            else:
                mate = other * 2 + (pos + 1) % 2
                send(name, buf.at[mate], mate)
        slots[name][pos] = buf[pos]

    def user_products(layer, item_panel):
        name = f"urs{layer}"
        buf = part_user.at[layer - 1]
        for off in (2, 1, 3, 0):
            other = (col + off) % 4
            rows = pl.ds(pl.multiple_of(other * 256, 256), 256)
            res = mm(item_panel, adj[rows, :], NT)
            if off:
                buf[other] = res
                send(name, buf.at[other], other)
            else:
                slots[name][col] = res

    def item_mid(layer):
        arrive(f"irs{layer}")
        val = total(f"irs{layer}")
        own_item[layer - 1] = val
        slots[f"izz{layer}"][zed] = val
        send_all(f"izz{layer}", own_item.at[layer - 1])

    tot_user = user_t.astype(F32)
    tot_item = emb_item_b[pos].astype(F32)

    def user_end(layer, tot):
        arrive(f"urs{layer}")
        val = total(f"urs{layer}").astype(BF16)
        tot = tot + val.astype(F32)
        res = val if layer < LAYERS else (tot * 0.25).astype(BF16)
        user_src[layer] = res
        slots[f"uag{layer}"][col] = res
        send_all(f"uag{layer}", user_src.at[layer])
        return tot

    def item_end(layer, tot):
        arrive(f"izz{layer}")
        val = total(f"izz{layer}").astype(BF16)
        tot = tot + val.astype(F32)
        res = val if layer < LAYERS else (tot * 0.25).astype(BF16)
        row_t[layer - 1] = res
        slots[f"iag{layer}"][pos] = res
        send_all(f"iag{layer}", row_t.at[layer - 1])
        return tot

    item_products(1, panel("emb_user"))
    user_products(1, panel("emb_item_b"))
    for layer in (1, 2):
        item_mid(layer)
        tot_user = user_end(layer, tot_user)
        arrive(f"uag{layer}")
        item_products(layer + 1, panel(f"uag{layer}"))
        tot_item = item_end(layer, tot_item)
        arrive(f"iag{layer}")
        user_products(layer + 1, panel(f"iag{layer}"))
    item_mid(3)
    user_end(3, tot_user)
    out_user_ref[...] = mm(eye(256, 256), user_src[3], NT).astype(BF16)
    arrive("uag3")
    picked_user = mm(panel("uag3"), hot_user[...], NT)
    item_end(3, tot_item)
    arrive("iag3")
    picked_item = mm(panel("iag3"), hot_item[...], NT)
    prod = picked_user * picked_item
    red = jnp.sum(prod, axis=0, keepdims=True)
    for k in range(8):
        marg[0, k:k + 1, :] = red[:, k * LANES:(k + 1) * LANES]
    loss_x[col] = marg[0]
    send_all("loss_x", marg.at[0])
    row_id = lax.broadcasted_iota(jnp.int32, (16, LANES), 0) + pos * 16
    col_id = lax.broadcasted_iota(jnp.int32, (16, LANES), 1)
    pick = jnp.where(row_id == col_id, 1.0, 0.0).astype(BF16)
    out_item_ref[...] = mm(pick, iag3[zed], NT).astype(BF16)
    arrive("loss_x")
    val = total("loss_x")
    marg[1] = val
    loss_yc[pos] = val
    send_all("loss_yc", marg.at[1])
    arrive("loss_yc")
    val = total("loss_yc")
    marg[2] = val
    loss_z[zed] = val
    send_all("loss_z", marg.at[2])
    arrive("loss_z")
    neg = -total("loss_z")
    loss_ref[...] = jnp.maximum(neg, 0.0) + jnp.log1p(jnp.exp(-jnp.abs(neg)))
    for name, _ in STAGES:
        whole(name).wait_send()


def solution(mesh):
    vm = pltpu.VMEM
    shapes = {
        "deg_user": ((4, 8, 128), F32), "deg_item_a": ((8, 8, 128), F32), "deg_item_b": ((8, 8, 128), F32),
        "emb_user": ((4, 64, 256), BF16), "emb_item_a": ((8, 16, 64), BF16), "emb_item_b": ((8, 64, 128), BF16),
    }
    for layer in (1, 2, 3):
        shapes[f"urs{layer}"] = ((4, 64, 256), F32)
        shapes[f"uag{layer}"] = ((4, 64, 256), BF16)
        shapes[f"irs{layer}"] = ((8, 64, 128), F32)
        shapes[f"izz{layer}"] = ((8, 64, 128), F32)
        shapes[f"iag{layer}"] = ((8, 64, 128), BF16)
    shapes["loss_x"] = ((4, 8, 128), F32)
    shapes["loss_yc"] = ((8, 8, 128), F32)
    shapes["loss_z"] = ((8, 8, 128), F32)
    scratch = [
        vm((1024, 1024), jnp.int32), vm((1024, 1024), BF16), vm((1024, 1024), BF16),
        vm((1024, 1024), BF16), vm((1024, 1024), BF16), vm((1024, 128), BF16),
        vm((1024, 128), F32), vm((8, 1024), F32), vm((3, 64, 128), BF16),
        vm((3, 8, 128), F32), vm((64, 128), BF16), vm((4, 64, 256), BF16),
        vm((3, 4, 64, 256), F32), vm((8, 128), F32), vm((3, 8, 64, 128), F32),
        vm((3, 64, 128), F32), vm((3, 8, 128), F32),
    ]
    scratch += [vm(*shapes[name]) for name, _ in STAGES]
    scratch += [pltpu.SemaphoreType.DMA((4,)), pltpu.SemaphoreType.DMA((len(STAGES),)),
                pltpu.SemaphoreType.DMA((len(STAGES),))]
    in_vmem = pl.BlockSpec(memory_space=pltpu.VMEM)
    call = pl.pallas_call(
        functools.partial(kernel, tuple(mesh.axis_names)),
        out_shape=(jax.ShapeDtypeStruct((256, 64), BF16), jax.ShapeDtypeStruct((16, 64), BF16),
                   jax.ShapeDtypeStruct((8, 128), F32)),
        in_specs=[pl.BlockSpec(memory_space=pl.ANY), in_vmem, in_vmem, in_vmem],
        out_specs=(in_vmem, in_vmem, in_vmem),
        scratch_shapes=scratch,
        compiler_params=pltpu.CompilerParams(collective_id=0, has_side_effects=True),
    )

    def device_body(mask_blk, user_shard, item_shard, triples):
        out_user, out_item, loss = call(mask_blk, user_shard, item_shard, triples)
        return out_user, out_item, loss.reshape(-1)

    return jax.shard_map(
        device_body,
        mesh=mesh,
        in_specs=(P("row", "col"), P(("row", "col"), None), P(("col", "row"), None), P()),
        out_specs=(P(("row", "col"), None), P(("col", "row"), None), P()),
        check_vma=False,
    )
```

```python
import functools

import jax
import jax.numpy as jnp
from jax import lax
from jax.experimental import pallas as pl
from jax.experimental.pallas import tpu as pltpu
from jax.sharding import PartitionSpec as P

LAYERS = 3
LANES = 128
F32 = jnp.float32
BF16 = jnp.bfloat16
I32 = jnp.int32
NT = (((1,), (1,)), ((), ()))
NN = (((1,), (0,)), ((), ()))

YC = (4, 5, 3, 2, 6, 7, 1)
X, Y, Z, YP, XYC = range(5)
SIZE = (4, 8, 8, 16, 32)
OFFSETS = (
    (2, 1, 3),
    YC,
    (4, 3, 5, 2, 6, 1, 7),
    tuple(8 + off for off in YC + (0,)) + YC,
    tuple(8 * dx + off for dx in (2, 1, 3, 0) for off in YC + (0,) if dx or off),
)
(DEG_USER, DEG_ITEM_A, DEG_ITEM_B, EMB_USER, EMB_ITEM_A, EMB_ITEM_B, LOSS_A, LOSS_Z) = range(8)
URS, UAG, IRS, IZZ, IAG = 7, 10, 13, 16, 19
STAGES = (
    (X, (8, 128), F32), (Y, (8, 128), F32), (Z, (8, 128), F32),
    (X, (64, 256), BF16), (Y, (16, 64), BF16), (Z, (64, 128), BF16),
    (XYC, (8, 128), F32), (Z, (8, 128), F32),
    *[(X, (64, 256), F32)] * 3, *[(X, (64, 256), BF16)] * 3,
    *[(Y, (64, 128), F32)] * 3, *[(Z, (32, 128), F32)] * 3, *[(YP, (32, 128), BF16)] * 3,
)
SCRATCH = (
    ((1024, 1024), I32), ((1024, 1024), BF16), ((1024, 1024), BF16),
    ((1024, 1024), BF16), ((1024, 1024), BF16), ((1024, 128), BF16),
    ((1024, 128), F32), ((8, 1024), F32), ((3, 8, 1024), I32),
    ((5, 8, 128), F32), ((64, 128), BF16), ((3, 64, 256), BF16),
    ((3, 4, 64, 256), F32), ((3, 8, 64, 128), F32),
    ((3, 64, 128), F32), ((3, 32, 128), BF16),
    ((64, 256), BF16), ((16, 64), BF16), ((3, 1024), I32),
)


class Stop(Exception):
    pass


def mm(lhs, rhs, dims):
    return lax.dot_general(lhs, rhs, dims, preferred_element_type=F32)


def eye(rows, cols):
    row_id = lax.broadcasted_iota(I32, (rows, cols), 0)
    col_id = lax.broadcasted_iota(I32, (rows, cols), 1)
    return jnp.where(row_id == col_id, 1.0, 0.0).astype(BF16)


def kernel(axis_names, stop, mask_hbm, user_hbm, item_hbm, trip_hbm, out_user_ref, out_item_ref, loss_ref, *refs):
    (mask_v, mask_b, adj, hot_user, hot_item, row_part, su_col, si_row, ids, small, item_tr, user_src,
     part_user, part_item, own_item, out_half, user_ref, item_ref, trip_ref) = refs[:len(SCRATCH)]
    slots = refs[len(SCRATCH):-3]
    load_sem, send_sem, recv_sem = refs[-3:]
    row = lax.axis_index("row")
    col = lax.axis_index("col")
    zed = row // 8
    pos = row % 8
    par = zed % 2
    here = (col, pos, zed, par * 8 + pos, col * 8 + pos)
    started, arrived, loads = [], [], []

    def device(group, idx):
        to_col, to_row = col, row
        if group == X:
            to_col = idx
        elif group == Y:
            to_row = zed * 8 + idx
        elif group == Z:
            to_row = idx * 8 + pos
        elif group == YP:
            to_row = (zed - par + idx // 8) * 8 + idx % 8
        else:
            to_col = idx // 8
            to_row = zed * 8 + idx % 8
        return tuple(to_col if name == "col" else to_row for name in axis_names)

    def peers(group):
        if group == YP:
            return [(par + off // 8) % 2 * 8 + (pos + off % 8) % 8 for off in OFFSETS[group]]
        if group == XYC:
            return [(col + off // 8) % 4 * 8 + (pos + off % 8) % 8 for off in OFFSETS[group]]
        return [(here[group] + off) % SIZE[group] for off in OFFSETS[group]]

    def send(stage, src, idx):
        if stage not in started:
            started.append(stage)
        group = STAGES[stage][0]
        pltpu.make_async_remote_copy(
            src_ref=src, dst_ref=slots[stage].at[here[group]],
            send_sem=send_sem.at[stage], recv_sem=recv_sem.at[stage],
            device_id=device(group, idx), device_id_type=pl.DeviceIdType.MESH).start()

    def send_all(stage, src):
        for idx in peers(STAGES[stage][0]):
            send(stage, src, idx)

    def whole(stage):
        group = STAGES[stage][0]
        part = slots[stage].at[pl.ds(0, SIZE[group] - 1)]
        return pltpu.make_async_remote_copy(
            src_ref=part, dst_ref=part, send_sem=send_sem.at[stage], recv_sem=recv_sem.at[stage],
            device_id=device(group, peers(group)[0]), device_id_type=pl.DeviceIdType.MESH)

    def arrive(stage):
        arrived.append(stage)
        whole(stage).wait_recv()

    def total(stage):
        buf = slots[stage]
        acc = buf[0]
        for idx in range(1, SIZE[STAGES[stage][0]]):
            acc = acc + buf[idx]
        return acc

    def panel(stage):
        buf = slots[stage]
        group = STAGES[stage][0]
        if group == YP:
            halves = [jnp.concatenate([buf[8 * k + idx] for idx in range(8)], axis=1) for k in (0, 1)]
            return jnp.concatenate(halves, axis=0)
        return jnp.concatenate([buf[idx] for idx in range(SIZE[group])], axis=1)

    def mark(point):
        if stop == point:
            raise Stop

    def lanes(k):
        return slice(k * LANES, (k + 1) * LANES)

    def load(src, dst):
        cp = pltpu.make_async_copy(src, dst, load_sem.at[len(loads)])
        cp.start()
        loads.append(cp)
        return cp

    def body():
        barrier = pltpu.get_barrier_semaphore()
        n_peers = 0
        for group in (Z, XYC, YP):
            for off, idx in zip(OFFSETS[group], peers(group), strict=True):
                if group != YP or off >= 8:
                    pl.semaphore_signal(barrier, inc=1, device_id=device(group, idx),
                                        device_id_type=pl.DeviceIdType.MESH)
                    n_peers += 1
        for q in range(4):
            rows = pl.ds(q * 256, 256)
            load(mask_hbm.at[rows], mask_v.at[rows])
        user_cp = load(user_hbm, user_ref)
        item_cp = load(item_hbm, item_ref)
        trip_cp = load(trip_hbm, trip_ref)

        if stop == 0:
            pl.semaphore_wait(barrier, n_peers)
            for cp in loads:
                cp.wait()
            raise Stop

        def degree_rows(blk, acc):
            base = pl.multiple_of(blk * 32, 32)
            m = mask_v[pl.ds(base, 32), :].astype(F32)
            mask_b[pl.ds(base, 32), :] = m.astype(BF16)
            part = m[:, lanes(0)]
            for k in range(1, 8):
                part = part + m[:, lanes(k)]
            row_part[pl.ds(base, 32), :] = part.astype(BF16)
            return acc + ((m[0:8] + m[8:16]) + (m[16:24] + m[24:32]))

        acc = jnp.zeros((8, 1024), F32)
        for q in range(4):
            loads[q].wait()
            acc = lax.fori_loop(q * 8, (q + 1) * 8, degree_rows, acc)
        col_sum = jnp.sum(acc, axis=0, keepdims=True)
        for k in range(8):
            small[0, k:k + 1, :] = col_sum[:, lanes(k)]
        slots[DEG_ITEM_A][pos] = small[0]
        row_sum = mm(jnp.ones((8, LANES), BF16), row_part[...], NT)
        for k in range(8):
            small[1, k:k + 1, :] = row_sum[0:1, lanes(k)]
        slots[DEG_USER][col] = small[1]
        for cp in (user_cp, item_cp, trip_cp):
            cp.wait()
        pl.semaphore_wait(barrier, n_peers)
        mark(1)
        send_all(DEG_ITEM_A, small.at[0])
        send_all(DEG_USER, small.at[1])
        mark(2)
        send_all(EMB_USER, user_ref)
        send_all(EMB_ITEM_A, item_ref)
        user_t = user_ref[...]
        slots[EMB_USER][col] = user_t
        slots[EMB_ITEM_A][pos] = item_ref[...]
        ids[0] = jnp.broadcast_to(trip_ref[0:1, :] - row * 1024, (8, 1024))
        ids[1] = jnp.broadcast_to(trip_ref[1:2, :] - col * 1024, (8, 1024))
        ids[2] = jnp.broadcast_to(trip_ref[2:3, :] - col * 1024, (8, 1024))

        def one_hot(blk, carry):
            base = pl.multiple_of(blk * 16, 16)
            for k in range(8):
                hits = []
                for half in range(2):
                    sub = lax.broadcasted_iota(I32, (8, LANES), 0) + (base + half * 8)
                    hits.append([jnp.where(ids[w, :, lanes(k)] == sub, 1.0, 0.0) for w in range(3)])
                hot_user[pl.ds(base, 16), lanes(k)] = jnp.concatenate([hit[0] for hit in hits], axis=0).astype(BF16)
                hot_item[pl.ds(base, 16), lanes(k)] = jnp.concatenate([hit[1] - hit[2] for hit in hits], axis=0).astype(BF16)
            return carry

        def item_columns(stage, layer, user_panel, prepare=None):
            buf = part_item.at[layer - 1]
            for off in (2, 1, 3, 0):
                other = (pos // 2 + off) % 4
                cols = pl.ds(pl.multiple_of(other * 256, 256), 256)
                if prepare is not None:
                    prepare(cols)
                res = mm(user_panel, adj[:, cols], NN)
                buf[other * 2] = res[:, lanes(0)]
                buf[other * 2 + 1] = res[:, lanes(1)]
                if off:
                    send(stage, buf.at[other * 2], other * 2)
                    send(stage, buf.at[other * 2 + 1], other * 2 + 1)
                else:
                    mate = other * 2 + (pos + 1) % 2
                    send(stage, buf.at[mate], mate)
            slots[stage][pos] = buf[pos]

        arrive(DEG_ITEM_A)
        deg_sum = total(DEG_ITEM_A)
        small[2] = deg_sum
        slots[DEG_ITEM_B][zed] = deg_sum
        send_all(DEG_ITEM_B, small.at[2])
        mark(3)
        arrive(EMB_ITEM_A)
        gathered = jnp.concatenate([slots[EMB_ITEM_A][k] for k in range(8)], axis=0)
        item_t = mm(eye(64, 64), gathered, NT).astype(BF16)
        item_tr[...] = item_t
        slots[EMB_ITEM_B][zed] = item_t
        send_all(EMB_ITEM_B, item_tr)
        arrive(DEG_USER)
        scale_user = lax.rsqrt(jnp.maximum(total(DEG_USER), 1.0))
        for k in range(8):
            su_col[pl.ds(k * LANES, LANES), :] = jnp.transpose(jnp.broadcast_to(scale_user[k:k + 1, :], (LANES, LANES)))
        lax.fori_loop(0, 64, one_hot, 0)
        arrive(EMB_USER)
        mark(4)
        arrive(DEG_ITEM_B)
        scale_item = lax.rsqrt(jnp.maximum(total(DEG_ITEM_B), 1.0))
        for k in range(8):
            si_row[:, lanes(k)] = jnp.broadcast_to(scale_item[k:k + 1, :], (8, LANES))

        def prepare(cols):
            si = si_row[:, cols]

            def build(blk, carry):
                base = pl.multiple_of(blk * 16, 16)
                su = su_col[pl.ds(base, 16), :]
                m = mask_b[pl.ds(base, 16), cols].astype(F32)
                for k in range(2):
                    si2 = jnp.concatenate([si[:, lanes(k)]] * 2, axis=0)
                    val = ((m[:, lanes(k)] * su) * si2).astype(BF16)
                    adj[pl.ds(base, 16), pl.ds(pl.multiple_of(cols.start + k * LANES, LANES), LANES)] = val
                return carry

            lax.fori_loop(0, 64, build, 0)

        def user_products(layer, item_panel):
            buf = part_user.at[layer - 1]
            for off in (2, 1, 3, 0):
                other = (col + off) % 4
                rows = pl.ds(pl.multiple_of(other * 256, 256), 256)
                res = mm(item_panel, adj[rows, :], NT)
                if off:
                    buf[other] = res
                    send(URS + layer, buf.at[other], other)
                else:
                    slots[URS + layer][col] = res

        def item_mid(layer):
            own = own_item.at[layer - 1]
            arrive(IRS + layer)
            own[...] = total(IRS + layer)
            for idx in peers(Z):
                send(IZZ + layer, own.at[pl.ds(pl.multiple_of(idx % 2 * 32, 32), 32)], idx)
            slots[IZZ + layer][zed] = own[pl.ds(pl.multiple_of(par * 32, 32), 32)]

        def finish(stage, to, keep, layer, tot, place):
            arrive(stage)
            val = total(stage).astype(BF16)
            tot = tot + val.astype(F32)
            res = val if layer < LAYERS else (tot * 0.25).astype(BF16)
            keep[layer - 1] = res
            slots[to][place] = res
            send_all(to, keep.at[layer - 1])
            return tot

        def user_end(layer, tot):
            return finish(URS + layer, UAG + layer, user_src, layer, tot, col)

        def item_end(layer, tot):
            return finish(IZZ + layer, IAG + layer, out_half, layer, tot, par * 8 + pos)

        tot_user = user_t.astype(F32)
        item_columns(IRS + 1, 1, panel(EMB_USER), prepare)
        mark(5)
        arrive(EMB_ITEM_B)
        tot_item = slots[EMB_ITEM_B][pos, pl.ds(pl.multiple_of(par * 32, 32), 32)].astype(F32)
        user_products(1, panel(EMB_ITEM_B))
        mark(6)
        item_mid(1)
        mark(7)
        tot_user = user_end(1, tot_user)
        arrive(UAG + 1)
        item_columns(IRS + 2, 2, panel(UAG + 1))
        mark(8)
        tot_item = item_end(1, tot_item)
        mark(9)
        item_mid(2)
        arrive(IAG + 1)
        user_products(2, panel(IAG + 1))
        mark(10)
        tot_item = item_end(2, tot_item)
        tot_user = user_end(2, tot_user)
        mark(11)
        arrive(UAG + 2)
        item_columns(IRS + 3, 3, panel(UAG + 2))
        mark(12)
        arrive(IAG + 2)
        user_products(3, panel(IAG + 2))
        item_mid(3)
        mark(13)
        user_end(3, tot_user)
        out_user_ref[...] = user_src[2]
        arrive(UAG + 3)
        picked_user = mm(panel(UAG + 3), hot_user[...], NN)
        item_end(3, tot_item)
        mark(14)
        arrive(IAG + 3)
        picked_item = mm(panel(IAG + 3), hot_item[...], NN)
        red = jnp.sum(picked_user * picked_item, axis=0, keepdims=True)
        for k in range(8):
            small[3, k:k + 1, :] = red[:, lanes(k)]
        slots[LOSS_A][col * 8 + pos] = small[3]
        send_all(LOSS_A, small.at[3])
        mark(15)
        row_id = lax.broadcasted_iota(I32, (16, LANES), 0) + pos * 16
        col_id = lax.broadcasted_iota(I32, (16, LANES), 1)
        pick = jnp.where(row_id == col_id, 1.0, 0.0).astype(BF16)
        block = jnp.concatenate([slots[IAG + 3][zed], slots[IAG + 3][8 + zed]], axis=0)
        out_item_ref[...] = mm(pick, block, NT).astype(BF16)
        arrive(LOSS_A)
        val = total(LOSS_A)
        small[4] = val
        slots[LOSS_Z][zed] = val
        send_all(LOSS_Z, small.at[4])
        arrive(LOSS_Z)
        neg = -total(LOSS_Z)
        loss_ref[...] = jnp.maximum(neg, 0.0) + jnp.log1p(jnp.exp(-jnp.abs(neg)))

    try:
        body()
    except Stop:
        pass
    for stage in started:
        if stage not in arrived:
            arrive(stage)
        whole(stage).wait_send()


def hand_over(user_in, item_in, loss_in, user_out, item_out, loss_out):
    user_out[...] = user_in[...]
    item_out[...] = item_in[...]
    loss_out[...] = loss_in[...]


def solution(mesh, stop=None):
    scratch = [pltpu.VMEM(*spec) for spec in SCRATCH]
    scratch += [pltpu.VMEM((SIZE[group],) + shape, dtype) for group, shape, dtype in STAGES]
    scratch += [pltpu.SemaphoreType.DMA((7,)), pltpu.SemaphoreType.DMA((len(STAGES),)),
                pltpu.SemaphoreType.DMA((len(STAGES),))]
    in_vmem = pl.BlockSpec(memory_space=pltpu.VMEM)
    outs = (jax.ShapeDtypeStruct((64, 256), BF16), jax.ShapeDtypeStruct((16, 64), BF16),
            jax.ShapeDtypeStruct((8, 128), F32))
    call = pl.pallas_call(
        functools.partial(kernel, tuple(mesh.axis_names), stop),
        out_shape=outs,
        in_specs=[pl.BlockSpec(memory_space=pl.ANY)] * 4,
        out_specs=(in_vmem, in_vmem, in_vmem),
        scratch_shapes=scratch,
        compiler_params=pltpu.CompilerParams(collective_id=0, has_side_effects=True),
    )
    pass_on = pl.pallas_call(hand_over, out_shape=outs, in_specs=[in_vmem] * 3, out_specs=(in_vmem,) * 3)

    def device_body(mask_blk, user_shard, item_shard, triples):
        out_user, out_item, loss = pass_on(*call(mask_blk, user_shard.T, item_shard, triples.T))
        return out_user.T, out_item, loss.reshape(-1)

    return jax.shard_map(
        device_body,
        mesh=mesh,
        in_specs=(P("row", "col"), P(("row", "col"), None), P(("col", "row"), None), P()),
        out_specs=(P(("row", "col"), None), P(("col", "row"), None), P()),
        check_vma=False,
    )
```

```python
import functools

import jax
import jax.numpy as jnp
from jax import lax
from jax.experimental import pallas as pl
from jax.experimental.pallas import tpu as pltpu
from jax.sharding import PartitionSpec as P

LAYERS = 3
LANES = 128
LOADS = 8
F32 = jnp.float32
BF16 = jnp.bfloat16
I32 = jnp.int32
NT = (((1,), (1,)), ((), ()))
NN = (((1,), (0,)), ((), ()))

YC = (4, 5, 3, 2, 6, 7, 1)
X, Y, Z, YP, XYC = range(5)
SIZE = (4, 8, 8, 16, 32)
OFFSETS = (
    (2, 1, 3),
    YC,
    (4, 3, 5, 2, 6, 1, 7),
    tuple(8 + off for off in YC + (0,)) + YC,
    tuple(8 * dx + off for dx in (2, 1, 3, 0) for off in YC + (0,) if dx or off),
)
(DEG_USER, DEG_ITEM_A, DEG_ITEM_B, EMB_USER, EMB_ITEM_A, EMB_ITEM_B, LOSS_A, LOSS_Z) = range(8)
URS, UAG, IRS, IZZ, IAG = 7, 10, 13, 16, 19
STAGES = (
    (X, (8, 128), F32), (Y, (8, 128), F32), (Z, (8, 128), F32),
    (X, (64, 256), BF16), (Y, (16, 64), BF16), (Z, (64, 128), BF16),
    (XYC, (8, 128), F32), (Z, (8, 128), F32),
    *[(X, (64, 256), F32)] * 3, *[(X, (64, 256), BF16)] * 3,
    *[(Y, (64, 128), F32)] * 3, *[(Z, (32, 128), F32)] * 3, *[(YP, (32, 128), BF16)] * 3,
)
SCRATCH = (
    ((1024, 1024), I32), ((1024, 1024), F32), ((1024, 1024), BF16),
    ((1024, 1024), BF16), ((1024, 1024), BF16), ((1024, 128), BF16),
    ((1024, 128), F32), ((8, 1024), F32), ((3, 8, 1024), I32),
    ((5, 8, 128), F32), ((64, 128), BF16), ((3, 64, 256), BF16),
    ((3, 4, 64, 256), F32), ((3, 8, 64, 128), F32),
    ((3, 64, 128), F32), ((3, 32, 128), BF16),
    ((64, 256), BF16), ((16, 64), BF16), ((3, 1024), I32), ((4, 64, 256), F32),
)


class Stop(Exception):
    pass


def mm(lhs, rhs, dims):
    return lax.dot_general(lhs, rhs, dims, preferred_element_type=F32)


def eye(rows, cols):
    row_id = lax.broadcasted_iota(I32, (rows, cols), 0)
    col_id = lax.broadcasted_iota(I32, (rows, cols), 1)
    return jnp.where(row_id == col_id, 1.0, 0.0).astype(BF16)


def kernel(axis_names, stop, mask_hbm, user_hbm, item_hbm, trip_hbm, out_user_ref, out_item_ref, loss_ref, *refs):
    (mask_v, mask_su, adj, hot_user, hot_item, row_part, su_col, si_row, ids, small, item_tr, user_src,
     part_user, part_item, own_item, out_half, user_ref, item_ref, trip_ref, picked) = refs[:len(SCRATCH)]
    slots = refs[len(SCRATCH):-3]
    load_sem, send_sem, recv_sem = refs[-3:]
    row = lax.axis_index("row")
    col = lax.axis_index("col")
    zed = row // 8
    pos = row % 8
    par = zed % 2
    here = (col, pos, zed, par * 8 + pos, col * 8 + pos)
    started, arrived, loads = [], [], []

    def device(group, idx):
        to_col, to_row = col, row
        if group == X:
            to_col = idx
        elif group == Y:
            to_row = zed * 8 + idx
        elif group == Z:
            to_row = idx * 8 + pos
        elif group == YP:
            to_row = (zed - par + idx // 8) * 8 + idx % 8
        else:
            to_col = idx // 8
            to_row = zed * 8 + idx % 8
        return tuple(to_col if name == "col" else to_row for name in axis_names)

    def peers(group):
        if group == YP:
            return [(par + off // 8) % 2 * 8 + (pos + off % 8) % 8 for off in OFFSETS[group]]
        if group == XYC:
            return [(col + off // 8) % 4 * 8 + (pos + off % 8) % 8 for off in OFFSETS[group]]
        return [(here[group] + off) % SIZE[group] for off in OFFSETS[group]]

    def send(stage, src, idx):
        if stage not in started:
            started.append(stage)
        group = STAGES[stage][0]
        pltpu.make_async_remote_copy(
            src_ref=src, dst_ref=slots[stage].at[here[group]],
            send_sem=send_sem.at[stage], recv_sem=recv_sem.at[stage],
            device_id=device(group, idx), device_id_type=pl.DeviceIdType.MESH).start()

    def send_all(stage, src):
        for idx in peers(STAGES[stage][0]):
            send(stage, src, idx)

    def whole(stage):
        group = STAGES[stage][0]
        part = slots[stage].at[pl.ds(0, SIZE[group] - 1)]
        return pltpu.make_async_remote_copy(
            src_ref=part, dst_ref=part, send_sem=send_sem.at[stage], recv_sem=recv_sem.at[stage],
            device_id=device(group, peers(group)[0]), device_id_type=pl.DeviceIdType.MESH)

    def arrive(stage):
        arrived.append(stage)
        whole(stage).wait_recv()

    def total(stage):
        buf = slots[stage]
        acc = buf[0]
        for idx in range(1, SIZE[STAGES[stage][0]]):
            acc = acc + buf[idx]
        return acc

    def panel(stage):
        buf = slots[stage]
        group = STAGES[stage][0]
        if group == YP:
            halves = [jnp.concatenate([buf[8 * k + idx] for idx in range(8)], axis=1) for k in (0, 1)]
            return jnp.concatenate(halves, axis=0)
        return jnp.concatenate([buf[idx] for idx in range(SIZE[group])], axis=1)

    def mark(point):
        if stop == point:
            raise Stop

    def lanes(k):
        return slice(k * LANES, (k + 1) * LANES)

    def load(src, dst):
        cp = pltpu.make_async_copy(src, dst, load_sem.at[len(loads)])
        cp.start()
        loads.append(cp)
        return cp

    def body():
        for q in range(LOADS):
            rows = pl.ds(q * (1024 // LOADS), 1024 // LOADS)
            load(mask_hbm.at[rows], mask_v.at[rows])
        user_cp = load(user_hbm, user_ref)
        item_cp = load(item_hbm, item_ref)
        trip_cp = load(trip_hbm, trip_ref)
        barrier = pltpu.get_barrier_semaphore()
        n_peers = 0
        for group in (Z, XYC, YP):
            for off, idx in zip(OFFSETS[group], peers(group), strict=True):
                if group != YP or off >= 8:
                    pl.semaphore_signal(barrier, inc=1, device_id=device(group, idx),
                                        device_id_type=pl.DeviceIdType.MESH)
                    n_peers += 1

        if stop == 0:
            pl.semaphore_wait(barrier, n_peers)
            for cp in loads:
                cp.wait()
            raise Stop

        def degree_rows(blk, acc):
            base = pl.multiple_of(blk * 32, 32)
            m = mask_v[pl.ds(base, 32), :].astype(F32)
            part = m[:, lanes(0)]
            for k in range(1, 8):
                part = part + m[:, lanes(k)]
            row_part[pl.ds(base, 32), :] = part.astype(BF16)
            return acc + ((m[0:8] + m[8:16]) + (m[16:24] + m[24:32]))

        acc = jnp.zeros((8, 1024), F32)
        trips = 32 // LOADS
        for q in range(LOADS):
            loads[q].wait()
            acc = lax.fori_loop(q * trips, (q + 1) * trips, degree_rows, acc)
        col_sum = jnp.sum(acc, axis=0, keepdims=True)
        for k in range(8):
            small[0, k:k + 1, :] = col_sum[:, lanes(k)]
        slots[DEG_ITEM_A][pos] = small[0]
        row_sum = mm(jnp.ones((8, LANES), BF16), row_part[...], NT)
        for k in range(8):
            small[1, k:k + 1, :] = row_sum[0:1, lanes(k)]
        slots[DEG_USER][col] = small[1]
        for cp in (user_cp, item_cp, trip_cp):
            cp.wait()
        pl.semaphore_wait(barrier, n_peers)
        mark(1)
        send_all(DEG_ITEM_A, small.at[0])
        send_all(DEG_USER, small.at[1])
        mark(2)
        send_all(EMB_USER, user_ref)
        send_all(EMB_ITEM_A, item_ref)
        user_t = user_ref[...]
        slots[EMB_USER][col] = user_t
        slots[EMB_ITEM_A][pos] = item_ref[...]
        ids[0] = jnp.broadcast_to(trip_ref[0:1, :] - row * 1024, (8, 1024))
        ids[1] = jnp.broadcast_to(trip_ref[1:2, :] - col * 1024, (8, 1024))
        ids[2] = jnp.broadcast_to(trip_ref[2:3, :] - col * 1024, (8, 1024))

        def one_hot(blk, carry):
            base = pl.multiple_of(blk * 16, 16)
            for k in range(8):
                hits = []
                for half in range(2):
                    sub = lax.broadcasted_iota(I32, (8, LANES), 0) + (base + half * 8)
                    hits.append([jnp.where(ids[w, :, lanes(k)] == sub, 1.0, 0.0) for w in range(3)])
                hot_user[pl.ds(base, 16), lanes(k)] = jnp.concatenate([hit[0] for hit in hits], axis=0).astype(BF16)
                hot_item[pl.ds(base, 16), lanes(k)] = jnp.concatenate([hit[1] - hit[2] for hit in hits], axis=0).astype(BF16)
            return carry

        def item_columns(stage, layer, user_panel, prepare=None):
            buf = part_item.at[layer - 1]
            for off in (2, 1, 3, 0):
                other = (pos // 2 + off) % 4
                cols = pl.ds(pl.multiple_of(other * 256, 256), 256)
                if prepare is not None:
                    prepare(cols)
                res = mm(user_panel, adj[:, cols], NN)
                buf[other * 2] = res[:, lanes(0)]
                buf[other * 2 + 1] = res[:, lanes(1)]
                if off:
                    send(stage, buf.at[other * 2], other * 2)
                    send(stage, buf.at[other * 2 + 1], other * 2 + 1)
                else:
                    mate = other * 2 + (pos + 1) % 2
                    send(stage, buf.at[mate], mate)
            slots[stage][pos] = buf[pos]

        arrive(DEG_ITEM_A)
        deg_sum = total(DEG_ITEM_A)
        small[2] = deg_sum
        slots[DEG_ITEM_B][zed] = deg_sum
        send_all(DEG_ITEM_B, small.at[2])
        mark(3)
        arrive(EMB_ITEM_A)
        gathered = jnp.concatenate([slots[EMB_ITEM_A][k] for k in range(8)], axis=0)
        item_t = mm(eye(64, 64), gathered, NT).astype(BF16)
        item_tr[...] = item_t
        slots[EMB_ITEM_B][zed] = item_t
        send_all(EMB_ITEM_B, item_tr)
        arrive(DEG_USER)
        scale_user = lax.rsqrt(jnp.maximum(total(DEG_USER), 1.0))
        for k in range(8):
            su_col[pl.ds(k * LANES, LANES), :] = jnp.transpose(jnp.broadcast_to(scale_user[k:k + 1, :], (LANES, LANES)))

        def scale_rows(blk, carry):
            base = pl.multiple_of(blk * 32, 32)
            su = su_col[pl.ds(base, 32), :]
            for k in range(8):
                mask_su[pl.ds(base, 32), lanes(k)] = mask_v[pl.ds(base, 32), lanes(k)].astype(F32) * su
            return carry

        lax.fori_loop(0, 32, scale_rows, 0)
        lax.fori_loop(0, 64, one_hot, 0)
        arrive(EMB_USER)
        mark(4)
        arrive(DEG_ITEM_B)
        scale_item = lax.rsqrt(jnp.maximum(total(DEG_ITEM_B), 1.0))
        for k in range(8):
            si_row[:, lanes(k)] = jnp.broadcast_to(scale_item[k:k + 1, :], (8, LANES))

        def prepare(cols):
            si = si_row[:, cols]

            def build(blk, carry):
                base = pl.multiple_of(blk * 128, 128)
                for k in range(8):
                    rows = pl.ds(pl.multiple_of(base + k * 16, 16), 16)
                    adj[rows, cols] = (mask_su[rows, cols] * jnp.concatenate([si, si], axis=0)).astype(BF16)
                return carry

            lax.fori_loop(0, 8, build, 0)

        def user_products(layer, item_panel):
            buf = part_user.at[layer - 1]
            for off in (2, 1, 3, 0):
                other = (col + off) % 4
                rows = pl.ds(pl.multiple_of(other * 256, 256), 256)
                res = mm(item_panel, adj[rows, :], NT)
                if off:
                    buf[other] = res
                    send(URS + layer, buf.at[other], other)
                else:
                    slots[URS + layer][col] = res

        def item_mid(layer):
            own = own_item.at[layer - 1]
            arrive(IRS + layer)
            own[...] = total(IRS + layer)
            for idx in peers(Z):
                send(IZZ + layer, own.at[pl.ds(pl.multiple_of(idx % 2 * 32, 32), 32)], idx)
            slots[IZZ + layer][zed] = own[pl.ds(pl.multiple_of(par * 32, 32), 32)]

        def finish(stage, to, keep, layer, tot, place):
            arrive(stage)
            val = total(stage).astype(BF16)
            tot = tot + val.astype(F32)
            res = val if layer < LAYERS else (tot * 0.25).astype(BF16)
            keep[layer - 1] = res
            slots[to][place] = res
            send_all(to, keep.at[layer - 1])
            return tot

        def user_end(layer, tot):
            return finish(URS + layer, UAG + layer, user_src, layer, tot, col)

        def item_end(layer, tot):
            return finish(IZZ + layer, IAG + layer, out_half, layer, tot, par * 8 + pos)

        tot_user = user_t.astype(F32)
        item_columns(IRS + 1, 1, panel(EMB_USER), prepare)
        mark(5)
        arrive(EMB_ITEM_B)
        tot_item = slots[EMB_ITEM_B][pos, pl.ds(pl.multiple_of(par * 32, 32), 32)].astype(F32)
        user_products(1, panel(EMB_ITEM_B))
        mark(6)
        item_mid(1)
        mark(7)
        tot_user = user_end(1, tot_user)
        tot_item = item_end(1, tot_item)
        mark(8)
        arrive(UAG + 1)
        item_columns(IRS + 2, 2, panel(UAG + 1))
        mark(9)
        arrive(IAG + 1)
        user_products(2, panel(IAG + 1))
        mark(10)
        item_mid(2)
        tot_user = user_end(2, tot_user)
        mark(11)
        tot_item = item_end(2, tot_item)
        arrive(UAG + 2)
        item_columns(IRS + 3, 3, panel(UAG + 2))
        mark(12)
        item_mid(3)
        arrive(IAG + 2)
        user_products(3, panel(IAG + 2))
        mark(13)
        item_end(3, tot_item)
        user_end(3, tot_user)
        out_user_ref[...] = user_src[2]
        arrive(UAG + 3)
        out_panel = panel(UAG + 3)
        for k in range(4):
            picked[k] = mm(out_panel, hot_user[:, k * 256:(k + 1) * 256], NN)
        mark(14)
        arrive(IAG + 3)
        out_panel = panel(IAG + 3)
        for k in range(4):
            prod = mm(out_panel, hot_item[:, k * 256:(k + 1) * 256], NN) * picked[k]
            red = jnp.sum(prod, axis=0, keepdims=True)
            small[3, 2 * k:2 * k + 1, :] = red[:, lanes(0)]
            small[3, 2 * k + 1:2 * k + 2, :] = red[:, lanes(1)]
        slots[LOSS_A][col * 8 + pos] = small[3]
        send_all(LOSS_A, small.at[3])
        mark(15)
        row_id = lax.broadcasted_iota(I32, (16, LANES), 0) + pos * 16
        col_id = lax.broadcasted_iota(I32, (16, LANES), 1)
        pick = jnp.where(row_id == col_id, 1.0, 0.0).astype(BF16)
        block = jnp.concatenate([slots[IAG + 3][zed], slots[IAG + 3][8 + zed]], axis=0)
        out_item_ref[...] = mm(pick, block, NT).astype(BF16)
        arrive(LOSS_A)
        val = total(LOSS_A)
        small[4] = val
        slots[LOSS_Z][zed] = val
        send_all(LOSS_Z, small.at[4])
        arrive(LOSS_Z)
        neg = -total(LOSS_Z)
        loss_ref[...] = jnp.maximum(neg, 0.0) + jnp.log1p(jnp.exp(-jnp.abs(neg)))

    try:
        body()
    except Stop:
        pass
    for stage in started:
        if stage not in arrived:
            arrive(stage)
        whole(stage).wait_send()


def hand_over(user_in, item_in, loss_in, user_out, item_out, loss_out, sems):
    pairs = ((user_in, user_out), (item_in, item_out), (loss_in, loss_out))
    copies = [pltpu.make_async_copy(src, dst, sems.at[k]) for k, (src, dst) in enumerate(pairs)]
    for cp in copies:
        cp.start()
    for cp in copies:
        cp.wait()


def solution(mesh, stop=None):
    scratch = [pltpu.VMEM(*spec) for spec in SCRATCH]
    scratch += [pltpu.VMEM((SIZE[group],) + shape, dtype) for group, shape, dtype in STAGES]
    scratch += [pltpu.SemaphoreType.DMA((LOADS + 3,)), pltpu.SemaphoreType.DMA((len(STAGES),)),
                pltpu.SemaphoreType.DMA((len(STAGES),))]
    in_vmem = pl.BlockSpec(memory_space=pltpu.VMEM)
    outs = (jax.ShapeDtypeStruct((64, 256), BF16), jax.ShapeDtypeStruct((16, 64), BF16),
            jax.ShapeDtypeStruct((8, 128), F32))
    call = pl.pallas_call(
        functools.partial(kernel, tuple(mesh.axis_names), stop),
        out_shape=tuple(pltpu.VMEM(out.shape, out.dtype) for out in outs),
        in_specs=[pl.BlockSpec(memory_space=pl.ANY)] * 4,
        out_specs=(in_vmem, in_vmem, in_vmem),
        scratch_shapes=scratch,
        compiler_params=pltpu.CompilerParams(collective_id=0, has_side_effects=True),
    )
    pass_on = pl.pallas_call(
        hand_over, out_shape=outs, in_specs=[in_vmem] * 3,
        out_specs=(pl.BlockSpec(memory_space=pl.ANY),) * 3,
        scratch_shapes=[pltpu.SemaphoreType.DMA((3,))],
    )

    def device_body(mask_blk, user_shard, item_shard, triples):
        held = call(mask_blk, user_shard.T, item_shard, triples.T)
        out_user, out_item, loss = pass_on(*[pltpu.with_memory_space_constraint(x, pltpu.VMEM) for x in held])
        return out_user.T, out_item, loss.reshape(-1)

    return jax.shard_map(
        device_body,
        mesh=mesh,
        in_specs=(P("row", "col"), P(("row", "col"), None), P(("col", "row"), None), P()),
        out_specs=(P(("row", "col"), None), P(("col", "row"), None), P()),
        check_vma=False,
    )
```

```python
import functools

import jax
import jax.numpy as jnp
from jax import lax
from jax.experimental import pallas as pl
from jax.experimental.pallas import tpu as pltpu
from jax.sharding import PartitionSpec as P

LAYERS = 3
LANES = 128
LOADS = 8
F32 = jnp.float32
BF16 = jnp.bfloat16
I32 = jnp.int32
NT = (((1,), (1,)), ((), ()))
NN = (((1,), (0,)), ((), ()))

DX = (2, 1, 3, 0)
DY = (2, 1, 3, 0)
DZ = (4, 3, 5, 2, 6, 1, 7, 0)
EVERY = ((3, 3), (3, 3))
PLANE = ((7, 7), (7, 7))
GATHER = ((0, 7), (4, 3))
SPREAD = ((8, 7), (0, 15))
ROW = (8, LANES)
HALF = (64, LANES)
QUARTER = (32, LANES)
BLOCK = (64, 256)
STAGES = (
    (4, ROW, F32, *EVERY), (8, ROW, F32, *GATHER), (8, ROW, F32, *SPREAD),
    (4, BLOCK, BF16, *EVERY), (8, (16, 64), BF16, *PLANE), (8, HALF, BF16, *PLANE),
    (1, BLOCK, BF16, (0, 1), (1, 0)), (32, ROW, F32, (0, 31), (16, 15)), (8, ROW, F32, *SPREAD),
    *[(8, HALF, F32, *GATHER)] * 6,
    *[(4, HALF, BF16, (4, 3), (0, 7))] * 6,
    *[(8, HALF, F32, *GATHER)] * 6,
    *[(8, QUARTER, F32, (0, 7), (0, 7))] * 6,
    *[(8, QUARTER, BF16, *SPREAD)] * 6,
)
(DEG_USER, DEG_ITEM_A, DEG_ITEM_B, EMB_USER, EMB_ITEM_A, EMB_ITEM_B, EMB_MATE, LOSS_A, LOSS_Z) = range(9)
URS, UAG, IRS, IZZ, IAG = range(7, 37, 6)


def layer_stage(kind, layer, half):
    return kind + 2 * layer + half


SQUARE = (1024, 1024)
SCRATCH = (
    (SQUARE, I32), (SQUARE, F32), (SQUARE, BF16), (SQUARE, BF16), (SQUARE, BF16), ((1024, LANES), BF16),
    ((1024, LANES), F32), ((8, 1024), F32), ((3, 8, 1024), I32), ((5, *ROW), F32), (HALF, BF16),
    ((6, 2, *HALF), BF16), ((6, 4, *HALF), F32), ((6, 4, *HALF), F32), ((6, *HALF), F32), ((6, *QUARTER), BF16),
    (BLOCK, BF16), ((16, 64), BF16), ((3, 1024), I32), ((4, *BLOCK), F32),
    ((2, 2, *HALF), F32), ((2, *QUARTER), F32),
)


def mm(lhs, rhs, dims):
    return lax.dot_general(lhs, rhs, dims, preferred_element_type=F32)


def eye(rows, cols):
    row_id = lax.broadcasted_iota(I32, (rows, cols), 0)
    col_id = lax.broadcasted_iota(I32, (rows, cols), 1)
    return jnp.where(row_id == col_id, 1.0, 0.0).astype(BF16)


def kernel(axis_names, mask_hbm, user_hbm, item_hbm, trip_hbm, out_user_ref, out_item_ref, loss_ref, *refs):
    (mask_v, mask_su, adj, hot_user, hot_item, row_part, su_col, si_row, ids, small, item_tr, user_src,
     part_user, part_item, own_item, out_half, user_ref, item_ref, trip_ref, picked,
     tot_user, tot_item) = refs[:len(SCRATCH)]
    slots = refs[len(SCRATCH):-3]
    load_sem, send_sem, recv_sem = refs[-3:]
    row = lax.axis_index("row")
    col = lax.axis_index("col")
    zed = row // 8
    pos = row % 8
    yy = pos // 2
    core = pos % 2
    par = zed % 2
    started, arrived, loads = [], [], []

    def only(which):
        return pl.when(core == which)

    def device(to_col, to_row):
        return tuple(to_col if name == "col" else to_row for name in axis_names)

    def at_x(dx, which=None):
        return (col + dx) % 4, row if which is None else row - core + which

    def at_y(dy, which):
        return col, zed * 8 + (yy + dy) % 4 * 2 + which

    def at_z(dz, which=None):
        return col, (zed + dz) % 8 * 8 + (pos if which is None else yy * 2 + which)

    def send(stage, slot, src, target):
        if stage not in started:
            started.append(stage)
        pltpu.make_async_remote_copy(
            src_ref=src, dst_ref=slots[stage].at[slot],
            send_sem=send_sem.at[stage], recv_sem=recv_sem.at[stage],
            device_id=device(*target), device_id_type=pl.DeviceIdType.MESH).start()

    def batch(stage, count):
        part = slots[stage].at[pl.ds(0, count)]
        return pltpu.make_async_remote_copy(
            src_ref=part, dst_ref=part, send_sem=send_sem.at[stage], recv_sem=recv_sem.at[stage],
            device_id=device(*at_x(1)), device_id_type=pl.DeviceIdType.MESH)

    def arrive(stage):
        arrived.append(stage)
        count = STAGES[stage][3]
        if count[0] == count[1]:
            batch(stage, count[0]).wait_recv()
        else:
            for which in (0, 1):
                if count[which]:
                    only(which)(batch(stage, count[which]).wait_recv)

    def arrive_one(stage):
        arrived.append(stage)
        batch(stage, STAGES[stage][3][1]).wait_recv()

    def sent(stage, which):
        left = STAGES[stage][4][which]
        while left:
            count = min(left, STAGES[stage][0])
            batch(stage, count).wait_send()
            left -= count

    def total(stage, first=0, last=None):
        buf = slots[stage]
        acc = buf[first]
        for idx in range(first + 1, last or STAGES[stage][0]):
            acc = acc + buf[idx]
        return acc

    def panel(stage):
        buf = slots[stage]
        return jnp.concatenate([buf[idx] for idx in range(STAGES[stage][0])], axis=1)

    def columns(kind, layer, picks):
        bufs = [slots[layer_stage(kind, layer, half)] for half in (0, 1)]
        return jnp.concatenate([buf[idx] for idx in picks for buf in bufs], axis=1)

    def user_panel(layer):
        return columns(UAG, layer, range(4))

    def item_panel(layer):
        return jnp.concatenate([columns(IAG, layer, range(4)), columns(IAG, layer, range(4, 8))], axis=0)

    def arrive_both(kind, layer):
        for half in (0, 1):
            arrive(layer_stage(kind, layer, half))

    def lanes(k):
        return slice(k * LANES, (k + 1) * LANES)

    def load(src, dst):
        cp = pltpu.make_async_copy(src, dst, load_sem.at[len(loads)])
        cp.start()
        loads.append(cp)
        return cp

    def to_owners(stage, slot, src, local):
        for dy in DY[:3]:
            send(stage, slot, src, at_y(dy, 1))
        only(0)(lambda: send(stage, slot, src, at_y(0, 1)))

        @only(1)
        def _():
            slots[stage][slot] = local

    def along_z(stage, src):
        for dz in DZ:
            for which in (0, 1):
                if dz or not which:
                    send(stage, zed, src, at_z(dz, which))

    def body():
        for q in range(LOADS):
            rows = pl.ds(q * (1024 // LOADS), 1024 // LOADS)
            load(mask_hbm.at[rows], mask_v.at[rows])
        user_cp = load(user_hbm, user_ref)
        item_cp = load(item_hbm, item_ref)
        trip_cp = load(trip_hbm, trip_ref)
        barrier = pltpu.get_barrier_semaphore()
        targets = [at_z(dz, which) for dz in DZ[:7] for which in (0, 1)]
        targets += [((col + dx) % 4, zed * 8 + (pos + off) % 8) for dx in DX for off in range(8) if dx or off]
        targets += [(col, (zed - par + 1 - par) * 8 + (yy + dy) % 4 * 2 + which) for dy in DY[:3] for which in (0, 1)]
        for target in targets:
            pl.semaphore_signal(barrier, inc=1, device_id=device(*target), device_id_type=pl.DeviceIdType.MESH)
        n_peers = len(targets)


        def degree_rows(blk, acc):
            base = pl.multiple_of(blk * 32, 32)
            m = mask_v[pl.ds(base, 32), :].astype(F32)
            part = m[:, lanes(0)]
            for k in range(1, 8):
                part = part + m[:, lanes(k)]
            row_part[pl.ds(base, 32), :] = part.astype(BF16)
            return acc + ((m[0:8] + m[8:16]) + (m[16:24] + m[24:32]))

        acc = jnp.zeros((8, 1024), F32)
        trips = 32 // LOADS
        for q in range(LOADS):
            loads[q].wait()
            acc = lax.fori_loop(q * trips, (q + 1) * trips, degree_rows, acc)
        col_sum = jnp.sum(acc, axis=0, keepdims=True)
        for k in range(8):
            small[0, k:k + 1, :] = col_sum[:, lanes(k)]
        row_sum = mm(jnp.ones((8, LANES), BF16), row_part[...], NT)
        for k in range(8):
            small[1, k:k + 1, :] = row_sum[0:1, lanes(k)]
        slots[DEG_USER][col] = small[1]
        for cp in (user_cp, item_cp, trip_cp):
            cp.wait()
        pl.semaphore_wait(barrier, n_peers)
        to_owners(DEG_ITEM_A, pos, small.at[0], small[0])
        for dx in DX[:3]:
            send(DEG_USER, col, small.at[1], at_x(dx))
        for dx in DX[:3]:
            send(EMB_USER, col, user_ref, at_x(dx))
        for off in (4, 5, 3, 2, 6, 7, 1):
            send(EMB_ITEM_A, pos, item_ref, (col, zed * 8 + (pos + off) % 8))
        only(0)(lambda: send(EMB_MATE, 0, user_ref, at_y(0, 1)))
        user_t = user_ref[...]
        slots[EMB_USER][col] = user_t
        slots[EMB_ITEM_A][pos] = item_ref[...]
        for k, block in enumerate((row, col, col)):
            ids[k] = jnp.broadcast_to(trip_ref[k:k + 1, :] - block * 1024, (8, 1024))

        def one_hot(blk, carry):
            base = pl.multiple_of(blk * 16, 16)
            for k in range(8):
                hits = []
                for half in range(2):
                    sub = lax.broadcasted_iota(I32, (8, LANES), 0) + (base + half * 8)
                    hits.append([jnp.where(ids[w, :, lanes(k)] == sub, 1.0, 0.0) for w in range(3)])
                hot_user[pl.ds(base, 16), lanes(k)] = jnp.concatenate([hit[0] for hit in hits], axis=0).astype(BF16)
                hot_item[pl.ds(base, 16), lanes(k)] = jnp.concatenate([hit[1] - hit[2] for hit in hits], axis=0).astype(BF16)
            return carry

        def spread_halves(kind, layer, slot, store, offsets, product, target):
            for off in offsets:
                res = product(off)
                for half in (0, 1):
                    buf = store.at[2 * (layer - 1) + half]
                    if off:
                        buf[off] = res[:, lanes(half)]
                        if not half:
                            send(layer_stage(kind, layer, half), slot, buf.at[off], target(off))
                    else:
                        @only(0)
                        def _():
                            buf[off] = res[:, lanes(half)]
                            if not half:
                                send(layer_stage(kind, layer, half), slot, buf.at[off], target(off))

                        @only(1)
                        def _():
                            slots[layer_stage(kind, layer, half)][slot] = res[:, lanes(half)]
            stage = layer_stage(kind, layer, 1)
            buf = store.at[2 * layer - 1]
            for off in offsets[:3]:
                send(stage, slot, buf.at[off], target(off))
            only(0)(lambda: send(stage, slot, buf.at[0], target(0)))

        def item_columns(layer, user_rows, prepare=None):
            def product(off):
                cols = pl.ds(pl.multiple_of((yy + off) % 4 * 256, 256), 256)
                if prepare is not None:
                    prepare(cols)
                return mm(user_rows, adj[:, cols], NN)

            spread_halves(IRS, layer, pos, part_item, DY, product, lambda off: at_y(off, 1))

        def user_products(layer, item_rows):
            def product(off):
                rows = pl.ds(pl.multiple_of((col + off) % 4 * 256, 256), 256)
                return mm(item_rows, adj[rows, :], NT)

            spread_halves(URS, layer, core * 4 + col, part_user, DX, product, lambda off: at_x(off, 1))

        @only(1)
        def _():
            arrive_one(DEG_ITEM_A)
            deg_sum = total(DEG_ITEM_A)
            small[2] = deg_sum
            slots[DEG_ITEM_B][zed] = deg_sum
            along_z(DEG_ITEM_B, small.at[2])

        arrive(EMB_ITEM_A)
        gathered = jnp.concatenate([slots[EMB_ITEM_A][k] for k in range(8)], axis=0)
        item_t = mm(eye(64, 64), gathered, NT).astype(BF16)
        item_tr[...] = item_t
        slots[EMB_ITEM_B][zed] = item_t
        for dz in DZ[:7]:
            send(EMB_ITEM_B, zed, item_tr, at_z(dz))
        arrive(DEG_USER)
        scale_user = lax.rsqrt(jnp.maximum(total(DEG_USER), 1.0))
        for k in range(8):
            su_col[pl.ds(k * LANES, LANES), :] = jnp.transpose(jnp.broadcast_to(scale_user[k:k + 1, :], (LANES, LANES)))

        def scale_rows(blk, carry):
            base = pl.multiple_of(blk * 32, 32)
            su = su_col[pl.ds(base, 32), :]
            for k in range(8):
                mask_su[pl.ds(base, 32), lanes(k)] = mask_v[pl.ds(base, 32), lanes(k)].astype(F32) * su
            return carry

        lax.fori_loop(0, 32, scale_rows, 0)
        lax.fori_loop(0, 64, one_hot, 0)
        arrive(EMB_USER)
        arrive(DEG_ITEM_B)
        scale_item = lax.rsqrt(jnp.maximum(total(DEG_ITEM_B), 1.0))
        for k in range(8):
            si_row[:, lanes(k)] = jnp.broadcast_to(scale_item[k:k + 1, :], (8, LANES))

        def prepare(cols):
            si = si_row[:, cols]

            def build(blk, carry):
                base = pl.multiple_of(blk * 128, 128)
                for k in range(8):
                    rows = pl.ds(pl.multiple_of(base + k * 16, 16), 16)
                    adj[rows, cols] = (mask_su[rows, cols] * jnp.concatenate([si, si], axis=0)).astype(BF16)
                return carry

            lax.fori_loop(0, 8, build, 0)

        def item_mid(layer, half):
            @only(1)
            def _():
                own = own_item.at[2 * (layer - 1) + half]
                stage = layer_stage(IRS, layer, half)
                arrive_one(stage)
                own[...] = total(stage)
                stage = layer_stage(IZZ, layer, half)
                for dz in DZ[:7]:
                    dims = pl.ds(pl.multiple_of((par + dz) % 2 * 32, 32), 32)
                    send(stage, zed, own.at[dims], at_z(dz))
                slots[stage][zed] = own[pl.ds(pl.multiple_of(par * 32, 32), 32)]

        def finish(val, tot, layer):
            tot[...] = tot[...] + val.astype(F32)
            return val if layer < LAYERS else (tot[...] * 0.25).astype(BF16)

        def user_end(layer, half):
            @only(1)
            def _():
                keep = user_src.at[2 * (layer - 1) + half]
                come = layer_stage(URS, layer, half)
                stage = layer_stage(UAG, layer, half)
                arrive_one(come)
                for which in (0, 1):
                    val = total(come, 4 * which, 4 * which + 4).astype(BF16)
                    res = finish(val, tot_user.at[which, half], layer)
                    keep[which] = res
                    for dx in DX:
                        if dx or not which:
                            send(stage, col, keep.at[which], at_x(dx, which))
                slots[stage][col] = res

        def item_end(layer, half):
            @only(1)
            def _():
                keep = out_half.at[2 * (layer - 1) + half]
                mine = par * 4 + yy
                come = layer_stage(IZZ, layer, half)
                stage = layer_stage(IAG, layer, half)
                arrive_one(come)
                res = finish(total(come).astype(BF16), tot_item.at[half], layer)
                keep[...] = res
                for plane in (zed - par + 1 - par, zed):
                    for dy in DY:
                        for which in (0, 1):
                            if plane is not zed or dy or not which:
                                send(stage, mine, keep, (col, plane * 8 + (yy + dy) % 4 * 2 + which))
                slots[stage][mine] = res

        item_columns(1, panel(EMB_USER), prepare)
        arrive(EMB_ITEM_B)
        user_products(1, panel(EMB_ITEM_B))

        @only(1)
        def _():
            arrive_one(EMB_MATE)
            dims = pl.ds(pl.multiple_of(par * 32, 32), 32)
            for half in (0, 1):
                tot_user[0, half] = slots[EMB_MATE][0, :, lanes(half)].astype(F32)
                tot_user[1, half] = user_t[:, lanes(half)].astype(F32)
                tot_item[half] = slots[EMB_ITEM_B][2 * yy + half, dims].astype(F32)

        for half in (0, 1):
            item_mid(1, half)
            user_end(1, half)
        for half in (0, 1):
            item_end(1, half)
        arrive_both(UAG, 1)
        item_columns(2, user_panel(1))
        arrive_both(IAG, 1)
        user_products(2, item_panel(1))
        for step in (item_mid, user_end, item_end):
            for half in (0, 1):
                step(2, half)
        arrive_both(UAG, 2)
        item_columns(3, user_panel(2))
        for half in (0, 1):
            item_mid(3, half)
        arrive_both(IAG, 2)
        user_products(3, item_panel(2))
        for step in (item_end, user_end):
            for half in (0, 1):
                step(3, half)
        arrive_both(UAG, 3)
        for half in (0, 1):
            out_user_ref[:, lanes(half)] = slots[layer_stage(UAG, 3, half)][col]
        out_panel = user_panel(3)
        for k in range(4):
            picked[k] = mm(out_panel, hot_user[:, k * 256:(k + 1) * 256], NN)
        arrive_both(IAG, 3)
        out_panel = item_panel(3)
        for k in range(4):
            prod = mm(out_panel, hot_item[:, k * 256:(k + 1) * 256], NN) * picked[k]
            red = jnp.sum(prod, axis=0, keepdims=True)
            small[3, 2 * k:2 * k + 1, :] = red[:, lanes(0)]
            small[3, 2 * k + 1:2 * k + 2, :] = red[:, lanes(1)]
        place = col * 8 + pos
        for dx in DX:
            for dy in DY:
                target = ((col + dx) % 4, zed * 8 + (yy + dy) % 4 * 2 + 1)
                if dx or dy:
                    send(LOSS_A, place, small.at[3], target)
                else:
                    only(0)(lambda: send(LOSS_A, place, small.at[3], target))

        @only(1)
        def _():
            slots[LOSS_A][place] = small[3]

        @only(1)
        def _():
            arrive_one(LOSS_A)
            val = total(LOSS_A)
            small[4] = val
            slots[LOSS_Z][zed] = val
            along_z(LOSS_Z, small.at[4])

        row_id = lax.broadcasted_iota(I32, (16, LANES), 0) + pos * 16
        col_id = lax.broadcasted_iota(I32, (16, LANES), 1)
        pick = jnp.where(row_id == col_id, 1.0, 0.0).astype(BF16)

        for half in (0, 1):
            @pl.when(par == half)
            def _():
                buf = slots[layer_stage(IAG, 3, half)]
                block = jnp.concatenate([buf[zed // 2], buf[4 + zed // 2]], axis=0)
                out_item_ref[...] = mm(pick, block, NT).astype(BF16)

        arrive(LOSS_Z)
        neg = -total(LOSS_Z)
        loss_ref[...] = jnp.maximum(neg, 0.0) + jnp.log1p(jnp.exp(-jnp.abs(neg)))

    body()
    for which in (0, 1):
        @only(which)
        def _():
            for stage in started:
                sent(stage, which)


def hand_over(user_in, item_in, loss_in, user_out, item_out, loss_out, sems):
    pairs = ((user_in, user_out), (item_in, item_out), (loss_in, loss_out))
    copies = [pltpu.make_async_copy(src, dst, sems.at[k]) for k, (src, dst) in enumerate(pairs)]
    for cp in copies:
        cp.start()
    for cp in copies:
        cp.wait()


def solution(mesh):
    scratch = [pltpu.VMEM(*spec) for spec in SCRATCH]
    scratch += [pltpu.VMEM((stage[0],) + stage[1], stage[2]) for stage in STAGES]
    scratch += [pltpu.SemaphoreType.DMA((LOADS + 3,)), pltpu.SemaphoreType.DMA((len(STAGES),)),
                pltpu.SemaphoreType.DMA((len(STAGES),))]
    in_vmem = pl.BlockSpec(memory_space=pltpu.VMEM)
    outs = (jax.ShapeDtypeStruct((64, 256), BF16), jax.ShapeDtypeStruct((16, 64), BF16),
            jax.ShapeDtypeStruct((8, 128), F32))
    call = pl.pallas_call(
        functools.partial(kernel, tuple(mesh.axis_names)),
        out_shape=tuple(pltpu.VMEM(out.shape, out.dtype) for out in outs),
        in_specs=[pl.BlockSpec(memory_space=pl.ANY)] * 4,
        out_specs=(in_vmem, in_vmem, in_vmem),
        scratch_shapes=scratch,
        compiler_params=pltpu.CompilerParams(collective_id=0, has_side_effects=True),
    )
    pass_on = pl.pallas_call(
        hand_over, out_shape=outs, in_specs=[in_vmem] * 3,
        out_specs=(pl.BlockSpec(memory_space=pl.ANY),) * 3,
        scratch_shapes=[pltpu.SemaphoreType.DMA((3,))],
    )

    def device_body(mask_blk, user_shard, item_shard, triples):
        held = call(mask_blk, user_shard.T, item_shard, triples.T)
        out_user, out_item, loss = pass_on(*[pltpu.with_memory_space_constraint(x, pltpu.VMEM) for x in held])
        return out_user.T, out_item, loss.reshape(-1)

    return jax.shard_map(
        device_body,
        mesh=mesh,
        in_specs=(P("row", "col"), P(("row", "col"), None), P(("col", "row"), None), P()),
        out_specs=(P(("row", "col"), None), P(("col", "row"), None), P()),
        check_vma=False,
    )
```

```python
import functools

import jax
import jax.numpy as jnp
from jax import lax
from jax.experimental import pallas as pl
from jax.experimental.pallas import tpu as pltpu
from jax.sharding import PartitionSpec as P

LAYERS = 3
LANES = 128
LOADS = 8
F32 = jnp.float32
BF16 = jnp.bfloat16
I32 = jnp.int32
NT = (((1,), (1,)), ((), ()))
NN = (((1,), (0,)), ((), ()))

DX = (2, 1, 3, 0)
DY = (2, 1, 3, 0)
DZ = (4, 3, 5, 2, 6, 1, 7, 0)
EVERY = ((3, 3), (3, 3))
PLANE = ((7, 7), (7, 7))
GATHER = ((0, 7), (4, 3))
SPREAD = ((8, 7), (0, 15))
ROW = (8, LANES)
HALF = (64, LANES)
QUARTER = (32, LANES)
BLOCK = (64, 256)
STAGES = (
    (4, ROW, F32, *EVERY), (8, ROW, F32, *GATHER), (8, ROW, F32, *SPREAD),
    (4, BLOCK, BF16, *EVERY), (8, (16, 64), BF16, *PLANE), (8, HALF, BF16, *PLANE),
    (1, BLOCK, BF16, (0, 1), (1, 0)), (32, ROW, F32, (0, 31), (16, 15)), (8, ROW, F32, *SPREAD),
    *[(8, HALF, F32, *GATHER)] * 6,
    *[(4, HALF, BF16, (4, 3), (0, 7))] * 6,
    *[(8, HALF, F32, *GATHER)] * 6,
    *[(8, QUARTER, F32, (0, 7), (0, 7))] * 6,
    *[(8, QUARTER, BF16, *SPREAD)] * 6,
)
(DEG_USER, DEG_ITEM_A, DEG_ITEM_B, EMB_USER, EMB_ITEM_A, EMB_ITEM_B, EMB_MATE, LOSS_A, LOSS_Z) = range(9)
URS, UAG, IRS, IZZ, IAG = range(7, 37, 6)


def layer_stage(kind, layer, half):
    return kind + 2 * layer + half


SQUARE = (1024, 1024)
SCRATCH = (
    (SQUARE, I32), (SQUARE, F32), (SQUARE, BF16), (SQUARE, BF16), (SQUARE, BF16), ((1024, LANES), BF16),
    ((1024, LANES), F32), ((8, 1024), F32), ((3, 8, 1024), I32), ((5, *ROW), F32), (HALF, BF16),
    ((6, 2, *HALF), BF16), ((6, 4, *HALF), F32), ((6, 4, *HALF), F32), ((6, *HALF), F32), ((6, *QUARTER), BF16),
    (BLOCK, BF16), ((16, 64), BF16), ((3, 1024), I32), ((4, *BLOCK), F32), ((4, *BLOCK), F32),
    ((2, 2, *HALF), F32), ((2, *QUARTER), F32),
)


def mm(lhs, rhs, dims):
    return lax.dot_general(lhs, rhs, dims, preferred_element_type=F32)


def eye(rows, cols):
    row_id = lax.broadcasted_iota(I32, (rows, cols), 0)
    col_id = lax.broadcasted_iota(I32, (rows, cols), 1)
    return jnp.where(row_id == col_id, 1.0, 0.0).astype(BF16)


def kernel(axis_names, mask_hbm, user_hbm, item_hbm, trip_hbm, out_user_ref, out_item_ref, loss_ref, *refs):
    (mask_v, mask_su, adj, hot_user, hot_item, row_part, su_col, si_row, ids, small, item_tr, user_src,
     part_user, part_item, own_item, out_half, user_ref, item_ref, trip_ref, picked, chosen,
     tot_user, tot_item) = refs[:len(SCRATCH)]
    slots = refs[len(SCRATCH):-3]
    load_sem, send_sem, recv_sem = refs[-3:]
    row = lax.axis_index("row")
    col = lax.axis_index("col")
    zed = row // 8
    pos = row % 8
    yy = pos // 2
    core = pos % 2
    par = zed % 2
    loads = []

    def only(which):
        return pl.when(core == which)

    def device(to_col, to_row):
        return tuple(to_col if name == "col" else to_row for name in axis_names)

    def at_x(dx, which=None):
        return (col + dx) % 4, row if which is None else row - core + which

    def at_y(dy, which):
        return col, zed * 8 + (yy + dy) % 4 * 2 + which

    def at_z(dz, which=None):
        return col, (zed + dz) % 8 * 8 + (pos if which is None else yy * 2 + which)

    def send(stage, slot, src, target):
        pltpu.make_async_remote_copy(
            src_ref=src, dst_ref=slots[stage].at[slot],
            send_sem=send_sem.at[stage], recv_sem=recv_sem.at[stage],
            device_id=device(*target), device_id_type=pl.DeviceIdType.MESH).start()

    def batch(stage, count):
        part = slots[stage].at[pl.ds(0, count)]
        return pltpu.make_async_remote_copy(
            src_ref=part, dst_ref=part, send_sem=send_sem.at[stage], recv_sem=recv_sem.at[stage],
            device_id=device(*at_x(1)), device_id_type=pl.DeviceIdType.MESH)

    def arrive(stage):
        count = STAGES[stage][3]
        if count[0] == count[1]:
            batch(stage, count[0]).wait_recv()
        else:
            for which in (0, 1):
                if count[which]:
                    only(which)(batch(stage, count[which]).wait_recv)

    def arrive_one(stage):
        batch(stage, STAGES[stage][3][1]).wait_recv()

    def sent(stage, which):
        left = STAGES[stage][4][which]
        while left:
            count = min(left, STAGES[stage][0])
            batch(stage, count).wait_send()
            left -= count

    def total(stage, first=0, last=None):
        buf = slots[stage]
        acc = buf[first]
        for idx in range(first + 1, last or STAGES[stage][0]):
            acc = acc + buf[idx]
        return acc

    def panel(stage):
        buf = slots[stage]
        return jnp.concatenate([buf[idx] for idx in range(STAGES[stage][0])], axis=1)

    def columns(kind, layer, picks):
        bufs = [slots[layer_stage(kind, layer, half)] for half in (0, 1)]
        return jnp.concatenate([buf[idx] for idx in picks for buf in bufs], axis=1)

    def user_panel(layer):
        return columns(UAG, layer, range(4))

    def item_panel(layer):
        return jnp.concatenate([columns(IAG, layer, range(4)), columns(IAG, layer, range(4, 8))], axis=0)

    def arrive_both(kind, layer):
        for half in (0, 1):
            arrive(layer_stage(kind, layer, half))

    def lanes(k):
        return slice(k * LANES, (k + 1) * LANES)

    def load(src, dst):
        cp = pltpu.make_async_copy(src, dst, load_sem.at[len(loads)])
        cp.start()
        loads.append(cp)
        return cp

    def to_owners(stage, slot, src, local):
        for dy in DY[:3]:
            send(stage, slot, src, at_y(dy, 1))
        only(0)(lambda: send(stage, slot, src, at_y(0, 1)))

        @only(1)
        def _():
            slots[stage][slot] = local

    def along_z(stage, src):
        for dz in DZ:
            for which in (0, 1):
                if dz or not which:
                    send(stage, zed, src, at_z(dz, which))

    def body():
        for q in range(LOADS):
            rows = pl.ds(q * (1024 // LOADS), 1024 // LOADS)
            load(mask_hbm.at[rows], mask_v.at[rows])
        user_cp = load(user_hbm, user_ref)
        item_cp = load(item_hbm, item_ref)
        trip_cp = load(trip_hbm, trip_ref)
        barrier = pltpu.get_barrier_semaphore()
        targets = [at_z(dz, which) for dz in DZ[:7] for which in (0, 1)]
        targets += [((col + dx) % 4, zed * 8 + (pos + off) % 8) for dx in DX for off in range(8) if dx or off]
        targets += [(col, (zed - par + 1 - par) * 8 + (yy + dy) % 4 * 2 + which) for dy in DY[:3] for which in (0, 1)]
        for target in targets:
            pl.semaphore_signal(barrier, inc=1, device_id=device(*target), device_id_type=pl.DeviceIdType.MESH)
        n_peers = len(targets)


        def degree_rows(blk, acc):
            base = pl.multiple_of(blk * 32, 32)
            m = mask_v[pl.ds(base, 32), :].astype(F32)
            part = m[:, lanes(0)]
            for k in range(1, 8):
                part = part + m[:, lanes(k)]
            row_part[pl.ds(base, 32), :] = part.astype(BF16)
            return acc + ((m[0:8] + m[8:16]) + (m[16:24] + m[24:32]))

        acc = jnp.zeros((8, 1024), F32)
        trips = 32 // LOADS
        for q in range(LOADS):
            loads[q].wait()
            acc = lax.fori_loop(q * trips, (q + 1) * trips, degree_rows, acc)
        col_sum = jnp.sum(acc, axis=0, keepdims=True)
        for k in range(8):
            small[0, k:k + 1, :] = col_sum[:, lanes(k)]
        row_sum = mm(jnp.ones((8, LANES), BF16), row_part[...], NT)
        for k in range(8):
            small[1, k:k + 1, :] = row_sum[0:1, lanes(k)]
        slots[DEG_USER][col] = small[1]
        for cp in (user_cp, item_cp, trip_cp):
            cp.wait()
        pl.semaphore_wait(barrier, n_peers)
        to_owners(DEG_ITEM_A, pos, small.at[0], small[0])
        for dx in DX[:3]:
            send(DEG_USER, col, small.at[1], at_x(dx))
        for dx in DX[:3]:
            send(EMB_USER, col, user_ref, at_x(dx))
        for off in (4, 5, 3, 2, 6, 7, 1):
            send(EMB_ITEM_A, pos, item_ref, (col, zed * 8 + (pos + off) % 8))
        only(0)(lambda: send(EMB_MATE, 0, user_ref, at_y(0, 1)))
        user_t = user_ref[...]
        slots[EMB_USER][col] = user_t
        slots[EMB_ITEM_A][pos] = item_ref[...]
        for k, block in enumerate((row, col, col)):
            ids[k] = jnp.broadcast_to(trip_ref[k:k + 1, :] - block * 1024, (8, 1024))

        def one_hot(blk, carry):
            base = pl.multiple_of(blk * 16, 16)
            base_item = base // 512 * LANES + base % 512 // LANES * 256 + base % LANES
            for k in range(8):
                hits = []
                for half in range(2):
                    sub = lax.broadcasted_iota(I32, ROW, 0) + half * 8
                    near = (sub + base, sub + base_item, sub + base_item)
                    hits.append([jnp.where(ids[w, :, lanes(k)] == near[w], 1.0, 0.0) for w in range(3)])
                hot_user[pl.ds(base, 16), lanes(k)] = jnp.concatenate([hit[0] for hit in hits], axis=0).astype(BF16)
                hot_item[pl.ds(base, 16), lanes(k)] = jnp.concatenate([hit[1] - hit[2] for hit in hits], axis=0).astype(BF16)
            return carry

        def spread_halves(kind, layer, slot, store, offsets, product, target):
            for off in offsets:
                res = product(off)
                for half in (0, 1):
                    buf = store.at[2 * (layer - 1) + half]
                    if off:
                        buf[off] = res[:, lanes(half)]
                        if not half:
                            send(layer_stage(kind, layer, half), slot, buf.at[off], target(off))
                    else:
                        @only(0)
                        def _():
                            buf[off] = res[:, lanes(half)]
                            if not half:
                                send(layer_stage(kind, layer, half), slot, buf.at[off], target(off))

                        @only(1)
                        def _():
                            slots[layer_stage(kind, layer, half)][slot] = res[:, lanes(half)]
            stage = layer_stage(kind, layer, 1)
            buf = store.at[2 * layer - 1]
            for off in offsets[:3]:
                send(stage, slot, buf.at[off], target(off))
            only(0)(lambda: send(stage, slot, buf.at[0], target(0)))

        def item_columns(layer, user_rows, prepare=None):
            def product(off):
                cols = pl.ds(pl.multiple_of((yy + off) % 4 * 256, 256), 256)
                if prepare is not None:
                    prepare(cols)
                return mm(user_rows, adj[:, cols], NN)

            spread_halves(IRS, layer, pos, part_item, DY, product, lambda off: at_y(off, 1))

        def user_products(layer, item_rows):
            def product(off):
                rows = pl.ds(pl.multiple_of((col + off) % 4 * 256, 256), 256)
                return mm(item_rows, adj[rows, :], NT)

            spread_halves(URS, layer, core * 4 + col, part_user, DX, product, lambda off: at_x(off, 1))

        @only(1)
        def _():
            arrive_one(DEG_ITEM_A)
            deg_sum = total(DEG_ITEM_A)
            small[2] = deg_sum
            slots[DEG_ITEM_B][zed] = deg_sum
            along_z(DEG_ITEM_B, small.at[2])

        arrive(EMB_ITEM_A)
        gathered = jnp.concatenate([slots[EMB_ITEM_A][k] for k in range(8)], axis=0)
        item_t = mm(eye(64, 64), gathered, NT).astype(BF16)
        item_tr[...] = item_t
        slots[EMB_ITEM_B][zed] = item_t
        for dz in DZ[:7]:
            send(EMB_ITEM_B, zed, item_tr, at_z(dz))
        arrive(DEG_USER)
        scale_user = lax.rsqrt(jnp.maximum(total(DEG_USER), 1.0))
        for k in range(8):
            su_col[pl.ds(k * LANES, LANES), :] = jnp.transpose(jnp.broadcast_to(scale_user[k:k + 1, :], (LANES, LANES)))

        def scale_rows(blk, carry):
            base = pl.multiple_of(blk * 32, 32)
            su = su_col[pl.ds(base, 32), :]
            for k in range(8):
                mask_su[pl.ds(base, 32), lanes(k)] = mask_v[pl.ds(base, 32), lanes(k)].astype(F32) * su
            return carry

        lax.fori_loop(0, 32, scale_rows, 0)
        lax.fori_loop(0, 64, one_hot, 0)
        arrive(EMB_USER)
        arrive(DEG_ITEM_B)
        scale_item = lax.rsqrt(jnp.maximum(total(DEG_ITEM_B), 1.0))
        for k in range(8):
            si_row[:, lanes(k)] = jnp.broadcast_to(scale_item[k:k + 1, :], (8, LANES))

        def prepare(cols):
            si = si_row[:, cols]

            def build(blk, carry):
                base = pl.multiple_of(blk * 128, 128)
                for k in range(8):
                    rows = pl.ds(pl.multiple_of(base + k * 16, 16), 16)
                    adj[rows, cols] = (mask_su[rows, cols] * jnp.concatenate([si, si], axis=0)).astype(BF16)
                return carry

            lax.fori_loop(0, 8, build, 0)

        def item_mid(layer, half):
            @only(1)
            def _():
                own = own_item.at[2 * (layer - 1) + half]
                stage = layer_stage(IRS, layer, half)
                arrive_one(stage)
                own[...] = total(stage)
                stage = layer_stage(IZZ, layer, half)
                for dz in DZ[:7]:
                    dims = pl.ds(pl.multiple_of((par + dz) % 2 * 32, 32), 32)
                    send(stage, zed, own.at[dims], at_z(dz))
                slots[stage][zed] = own[pl.ds(pl.multiple_of(par * 32, 32), 32)]

        def finish(val, tot, layer):
            tot[...] = tot[...] + val.astype(F32)
            return val if layer < LAYERS else (tot[...] * 0.25).astype(BF16)

        def user_end(layer, half):
            @only(1)
            def _():
                keep = user_src.at[2 * (layer - 1) + half]
                come = layer_stage(URS, layer, half)
                stage = layer_stage(UAG, layer, half)
                arrive_one(come)
                for which in (0, 1):
                    val = total(come, 4 * which, 4 * which + 4).astype(BF16)
                    res = finish(val, tot_user.at[which, half], layer)
                    keep[which] = res
                    for dx in DX:
                        if dx or not which:
                            send(stage, col, keep.at[which], at_x(dx, which))
                slots[stage][col] = res

        def item_end(layer, half):
            @only(1)
            def _():
                keep = out_half.at[2 * (layer - 1) + half]
                mine = par * 4 + yy
                come = layer_stage(IZZ, layer, half)
                stage = layer_stage(IAG, layer, half)
                arrive_one(come)
                res = finish(total(come).astype(BF16), tot_item.at[half], layer)
                keep[...] = res
                for which in (0, 1):
                    for plane in (zed - par + 1 - par, zed):
                        for dy in DY:
                            if plane is not zed or dy or not which:
                                send(stage, mine, keep, (col, plane * 8 + (yy + dy) % 4 * 2 + which))
                slots[stage][mine] = res

        item_columns(1, panel(EMB_USER), prepare)
        arrive(EMB_ITEM_B)
        user_products(1, panel(EMB_ITEM_B))

        @only(1)
        def _():
            arrive_one(EMB_MATE)
            dims = pl.ds(pl.multiple_of(par * 32, 32), 32)
            for half in (0, 1):
                tot_user[0, half] = slots[EMB_MATE][0, :, lanes(half)].astype(F32)
                tot_user[1, half] = user_t[:, lanes(half)].astype(F32)
                tot_item[half] = slots[EMB_ITEM_B][2 * yy + half, dims].astype(F32)

        for step in (item_mid, user_end):
            for half in (0, 1):
                step(1, half)
        for half in (0, 1):
            item_end(1, half)
        arrive_both(UAG, 1)
        item_columns(2, user_panel(1))
        arrive_both(IAG, 1)
        user_products(2, item_panel(1))
        for step in (item_mid, user_end, item_end):
            for half in (0, 1):
                step(2, half)
        arrive_both(UAG, 2)
        item_columns(3, user_panel(2))
        arrive_both(IAG, 2)
        user_products(3, item_panel(2))
        for half in (0, 1):
            item_mid(3, half)
        for step in (user_end, item_end):
            for half in (0, 1):
                step(3, half)
        arrive_both(UAG, 3)
        for half in (0, 1):
            out_user_ref[:, lanes(half)] = slots[layer_stage(UAG, 3, half)][col]
        out_panel = user_panel(3)
        for k in range(4):
            picked[k] = mm(out_panel, hot_user[:, k * 256:(k + 1) * 256], NN)
        def item_half(half):
            stage = layer_stage(IAG, LAYERS, half)
            arrive(stage)
            rows = [jnp.concatenate([slots[stage][k + idx] for idx in range(4)], axis=1) for k in (0, 4)]
            return jnp.concatenate(rows, axis=0)

        first = item_half(0)
        for k in range(4):
            chosen[k] = mm(first, hot_item[:512, k * 256:(k + 1) * 256], NN)
        second = item_half(1)
        for k in range(4):
            prod = (chosen[k] + mm(second, hot_item[512:, k * 256:(k + 1) * 256], NN)) * picked[k]
            red = jnp.sum(prod, axis=0, keepdims=True)
            for half in (0, 1):
                small[3, 2 * k + half:2 * k + half + 1, :] = red[:, lanes(half)]
        place = col * 8 + pos
        for dx in DX:
            for dy in DY:
                target = ((col + dx) % 4, zed * 8 + (yy + dy) % 4 * 2 + 1)
                if dx or dy:
                    send(LOSS_A, place, small.at[3], target)
                else:
                    only(0)(lambda: send(LOSS_A, place, small.at[3], target))

        @only(1)
        def _():
            slots[LOSS_A][place] = small[3]

        @only(1)
        def _():
            arrive_one(LOSS_A)
            val = total(LOSS_A)
            small[4] = val
            slots[LOSS_Z][zed] = val
            along_z(LOSS_Z, small.at[4])

        row_id = lax.broadcasted_iota(I32, (16, LANES), 0) + pos * 16
        col_id = lax.broadcasted_iota(I32, (16, LANES), 1)
        pick = jnp.where(row_id == col_id, 1.0, 0.0).astype(BF16)

        for half in (0, 1):
            @pl.when(par == half)
            def _():
                buf = slots[layer_stage(IAG, 3, half)]
                block = jnp.concatenate([buf[zed // 2], buf[4 + zed // 2]], axis=0)
                out_item_ref[...] = mm(pick, block, NT).astype(BF16)

        for which in (0, 1):
            @only(which)
            def _():
                for stage in range(len(STAGES)):
                    sent(stage, which)

        arrive(LOSS_Z)
        neg = -total(LOSS_Z)
        loss_ref[...] = jnp.maximum(neg, 0.0) + jnp.log1p(jnp.exp(-jnp.abs(neg)))

    body()


def hand_over(user_in, item_in, loss_in, user_out, item_out, loss_out, sems):
    pairs = ((user_in, user_out), (item_in, item_out), (loss_in, loss_out))
    copies = [pltpu.make_async_copy(src, dst, sems.at[k]) for k, (src, dst) in enumerate(pairs)]
    for cp in copies:
        cp.start()
    for cp in copies:
        cp.wait()


def solution(mesh):
    scratch = [pltpu.VMEM(*spec) for spec in SCRATCH]
    scratch += [pltpu.VMEM((stage[0],) + stage[1], stage[2]) for stage in STAGES]
    scratch += [pltpu.SemaphoreType.DMA((LOADS + 3,)), pltpu.SemaphoreType.DMA((len(STAGES),)),
                pltpu.SemaphoreType.DMA((len(STAGES),))]
    in_vmem = pl.BlockSpec(memory_space=pltpu.VMEM)
    outs = (jax.ShapeDtypeStruct((64, 256), BF16), jax.ShapeDtypeStruct((16, 64), BF16),
            jax.ShapeDtypeStruct((8, 128), F32))
    call = pl.pallas_call(
        functools.partial(kernel, tuple(mesh.axis_names)),
        out_shape=tuple(pltpu.VMEM(out.shape, out.dtype) for out in outs),
        in_specs=[pl.BlockSpec(memory_space=pl.ANY)] * 4,
        out_specs=(in_vmem, in_vmem, in_vmem),
        scratch_shapes=scratch,
        compiler_params=pltpu.CompilerParams(collective_id=0, has_side_effects=True),
    )
    pass_on = pl.pallas_call(
        hand_over, out_shape=outs, in_specs=[in_vmem] * 3,
        out_specs=(pl.BlockSpec(memory_space=pl.ANY),) * 3,
        scratch_shapes=[pltpu.SemaphoreType.DMA((3,))],
    )

    def device_body(mask_blk, user_shard, item_shard, triples):
        held = call(mask_blk, user_shard.T, item_shard, triples.T)
        out_user, out_item, loss = pass_on(*[pltpu.with_memory_space_constraint(x, pltpu.VMEM) for x in held])
        return out_user.T, out_item, loss.reshape(-1)

    return jax.shard_map(
        device_body,
        mesh=mesh,
        in_specs=(P("row", "col"), P(("row", "col"), None), P(("col", "row"), None), P()),
        out_specs=(P(("row", "col"), None), P(("col", "row"), None), P()),
        check_vma=False,
    )
```

```python
import functools

import jax
import jax.numpy as jnp
from jax import lax
from jax.experimental import pallas as pl
from jax.experimental.pallas import tpu as pltpu
from jax.sharding import PartitionSpec as P

LAYERS = 3
LANES = 128
LOADS = 8
F32 = jnp.float32
BF16 = jnp.bfloat16
I32 = jnp.int32
NT = (((1,), (1,)), ((), ()))
NN = (((1,), (0,)), ((), ()))

DX = (2, 1, 3, 0)
DY = (2, 1, 3, 0)
DZ = (4, 3, 5, 2, 6, 1, 7, 0)
EVERY = ((3, 3), (3, 3))
PLANE = ((7, 7), (7, 7))
GATHER = ((0, 7), (4, 3))
SPREAD = ((8, 7), (0, 15))
ROW = (8, LANES)
HALF = (64, LANES)
QUARTER = (32, LANES)
BLOCK = (64, 256)
STAGES = (
    (4, ROW, F32, *EVERY), (8, ROW, F32, *GATHER), (8, ROW, F32, *SPREAD),
    (4, BLOCK, BF16, *EVERY), (8, (16, 64), BF16, *PLANE), (8, HALF, BF16, *PLANE),
    (1, BLOCK, BF16, (0, 1), (1, 0)), (32, ROW, F32, (0, 31), (16, 15)), (8, ROW, F32, *SPREAD),
    *[(8, HALF, F32, *GATHER)] * 6,
    *[(4, HALF, BF16, (4, 3), (0, 7))] * 6,
    *[(8, HALF, F32, *GATHER)] * 6,
    *[(8, QUARTER, F32, (0, 7), (0, 7))] * 6,
    *[(8, QUARTER, BF16, *SPREAD)] * 6,
)
(DEG_USER, DEG_ITEM_A, DEG_ITEM_B, EMB_USER, EMB_ITEM_A, EMB_ITEM_B, EMB_MATE, LOSS_A, LOSS_Z) = range(9)
URS, UAG, IRS, IZZ, IAG = range(7, 37, 6)


def layer_stage(kind, layer, half):
    return kind + 2 * layer + half


SQUARE = (1024, 1024)
SCRATCH = (
    (SQUARE, I32), (SQUARE, F32), (SQUARE, BF16), (SQUARE, BF16), (SQUARE, BF16), ((1024, LANES), BF16),
    ((1024, LANES), F32), ((8, 1024), F32), ((3, 8, 1024), I32), ((5, *ROW), F32), (HALF, BF16),
    ((6, 2, *HALF), BF16), ((6, 4, *HALF), F32), ((6, 4, *HALF), F32), ((6, *HALF), F32), ((6, *QUARTER), BF16),
    (BLOCK, BF16), ((16, 64), BF16), ((3, 1024), I32), ((4, *BLOCK), F32), ((4, *BLOCK), F32),
    ((2, 2, *HALF), F32), ((2, *QUARTER), F32),
)


def mm(lhs, rhs, dims):
    return lax.dot_general(lhs, rhs, dims, preferred_element_type=F32)


def eye(rows, cols):
    row_id = lax.broadcasted_iota(I32, (rows, cols), 0)
    col_id = lax.broadcasted_iota(I32, (rows, cols), 1)
    return jnp.where(row_id == col_id, 1.0, 0.0).astype(BF16)


def kernel(axis_names, mask_hbm, user_hbm, item_hbm, trip_hbm, out_user_ref, out_item_ref, loss_ref, *refs):
    (mask_v, mask_su, adj, hot_user, hot_item, row_part, su_col, si_row, ids, small, item_tr, user_src,
     part_user, part_item, own_item, out_half, user_ref, item_ref, trip_ref, picked, chosen,
     tot_user, tot_item) = refs[:len(SCRATCH)]
    slots = refs[len(SCRATCH):-3]
    load_sem, send_sem, recv_sem = refs[-3:]
    row = lax.axis_index("row")
    col = lax.axis_index("col")
    zed = row // 8
    pos = row % 8
    yy = pos // 2
    core = pos % 2
    par = zed % 2
    loads = []

    def only(which):
        return pl.when(core == which)

    def device(to_col, to_row):
        return tuple(to_col if name == "col" else to_row for name in axis_names)

    def at_x(dx, which=None):
        return (col + dx) % 4, row if which is None else row - core + which

    def at_y(dy, which):
        return col, zed * 8 + (yy + dy) % 4 * 2 + which

    def at_z(dz, which=None):
        return col, (zed + dz) % 8 * 8 + (pos if which is None else yy * 2 + which)

    def send(stage, slot, src, target):
        pltpu.make_async_remote_copy(
            src_ref=src, dst_ref=slots[stage].at[slot],
            send_sem=send_sem.at[stage], recv_sem=recv_sem.at[stage],
            device_id=device(*target), device_id_type=pl.DeviceIdType.MESH).start()

    def batch(stage, count):
        part = slots[stage].at[pl.ds(0, count)]
        return pltpu.make_async_remote_copy(
            src_ref=part, dst_ref=part, send_sem=send_sem.at[stage], recv_sem=recv_sem.at[stage],
            device_id=device(*at_x(1)), device_id_type=pl.DeviceIdType.MESH)

    def arrive(stage):
        count = STAGES[stage][3]
        if count[0] == count[1]:
            batch(stage, count[0]).wait_recv()
        else:
            for which in (0, 1):
                if count[which]:
                    only(which)(batch(stage, count[which]).wait_recv)

    def arrive_one(stage):
        batch(stage, STAGES[stage][3][1]).wait_recv()

    def sent(stage, which):
        left = STAGES[stage][4][which]
        while left:
            count = min(left, STAGES[stage][0])
            batch(stage, count).wait_send()
            left -= count

    def total(stage, first=0, last=None):
        buf = slots[stage]
        acc = buf[first]
        for idx in range(first + 1, last or STAGES[stage][0]):
            acc = acc + buf[idx]
        return acc

    def panel(stage):
        buf = slots[stage]
        return jnp.concatenate([buf[idx] for idx in range(STAGES[stage][0])], axis=1)

    def columns(kind, layer, picks):
        bufs = [slots[layer_stage(kind, layer, half)] for half in (0, 1)]
        return jnp.concatenate([buf[idx] for idx in picks for buf in bufs], axis=1)

    def user_panel(layer):
        return columns(UAG, layer, range(4))

    def arrive_both(kind, layer):
        for half in (0, 1):
            arrive(layer_stage(kind, layer, half))

    def lanes(k):
        return slice(k * LANES, (k + 1) * LANES)

    def load(src, dst):
        cp = pltpu.make_async_copy(src, dst, load_sem.at[len(loads)])
        cp.start()
        loads.append(cp)
        return cp

    def to_owners(stage, slot, src, local):
        for dy in DY[:3]:
            send(stage, slot, src, at_y(dy, 1))
        only(0)(lambda: send(stage, slot, src, at_y(0, 1)))

        @only(1)
        def _():
            slots[stage][slot] = local

    def along_z(stage, src):
        for dz in DZ:
            for which in (0, 1):
                if dz or not which:
                    send(stage, zed, src, at_z(dz, which))

    def body():
        for q in range(LOADS):
            rows = pl.ds(q * (1024 // LOADS), 1024 // LOADS)
            load(mask_hbm.at[rows], mask_v.at[rows])
        user_cp = load(user_hbm, user_ref)
        item_cp = load(item_hbm, item_ref)
        trip_cp = load(trip_hbm, trip_ref)
        barrier = pltpu.get_barrier_semaphore()
        targets = [at_z(dz, which) for dz in DZ[:7] for which in (0, 1)]
        targets += [((col + dx) % 4, zed * 8 + (pos + off) % 8) for dx in DX for off in range(8) if dx or off]
        targets += [(col, (zed - par + 1 - par) * 8 + (yy + dy) % 4 * 2 + which) for dy in DY[:3] for which in (0, 1)]
        for target in targets:
            pl.semaphore_signal(barrier, inc=1, device_id=device(*target), device_id_type=pl.DeviceIdType.MESH)
        n_peers = len(targets)


        def degree_rows(blk, acc):
            base = pl.multiple_of(blk * 32, 32)
            m = mask_v[pl.ds(base, 32), :].astype(F32)
            part = m[:, lanes(0)]
            for k in range(1, 8):
                part = part + m[:, lanes(k)]
            row_part[pl.ds(base, 32), :] = part.astype(BF16)
            return acc + ((m[0:8] + m[8:16]) + (m[16:24] + m[24:32]))

        acc = jnp.zeros((8, 1024), F32)
        trips = 32 // LOADS
        for q in range(LOADS):
            loads[q].wait()
            acc = lax.fori_loop(q * trips, (q + 1) * trips, degree_rows, acc)
        col_sum = jnp.sum(acc, axis=0, keepdims=True)
        for k in range(8):
            small[0, k:k + 1, :] = col_sum[:, lanes(k)]
        row_sum = mm(jnp.ones((8, LANES), BF16), row_part[...], NT)
        for k in range(8):
            small[1, k:k + 1, :] = row_sum[0:1, lanes(k)]
        slots[DEG_USER][col] = small[1]
        for cp in (user_cp, item_cp, trip_cp):
            cp.wait()
        pl.semaphore_wait(barrier, n_peers)
        to_owners(DEG_ITEM_A, pos, small.at[0], small[0])
        for dx in DX[:3]:
            send(DEG_USER, col, small.at[1], at_x(dx))
        for dx in DX[:3]:
            send(EMB_USER, col, user_ref, at_x(dx))
        for off in (4, 5, 3, 2, 6, 7, 1):
            send(EMB_ITEM_A, pos, item_ref, (col, zed * 8 + (pos + off) % 8))
        only(0)(lambda: send(EMB_MATE, 0, user_ref, at_y(0, 1)))
        user_t = user_ref[...]
        slots[EMB_USER][col] = user_t
        slots[EMB_ITEM_A][pos] = item_ref[...]
        for k, block in enumerate((row, col, col)):
            ids[k] = jnp.broadcast_to(trip_ref[k:k + 1, :] - block * 1024, (8, 1024))

        def one_hot(blk, carry):
            base = pl.multiple_of(blk * 16, 16)
            base_item = base // 512 * LANES + base % 512 // LANES * 256 + base % LANES
            for k in range(8):
                hits = []
                for half in range(2):
                    sub = lax.broadcasted_iota(I32, ROW, 0) + half * 8
                    near = (sub + base, sub + base_item, sub + base_item)
                    hits.append([jnp.where(ids[w, :, lanes(k)] == near[w], 1.0, 0.0) for w in range(3)])
                hot_user[pl.ds(base, 16), lanes(k)] = jnp.concatenate([hit[0] for hit in hits], axis=0).astype(BF16)
                hot_item[pl.ds(base, 16), lanes(k)] = jnp.concatenate([hit[1] - hit[2] for hit in hits], axis=0).astype(BF16)
            return carry

        def spread_halves(kind, layer, slot, store, offsets, product, target):
            for off in offsets:
                res = product(off)
                for half in (0, 1):
                    buf = store.at[2 * (layer - 1) + half]
                    if off:
                        buf[off] = res[:, lanes(half)]
                        if not half:
                            send(layer_stage(kind, layer, half), slot, buf.at[off], target(off))
                    else:
                        @only(0)
                        def _():
                            buf[off] = res[:, lanes(half)]
                            if not half:
                                send(layer_stage(kind, layer, half), slot, buf.at[off], target(off))

                        @only(1)
                        def _():
                            slots[layer_stage(kind, layer, half)][slot] = res[:, lanes(half)]
            stage = layer_stage(kind, layer, 1)
            buf = store.at[2 * layer - 1]
            for off in offsets[:3]:
                send(stage, slot, buf.at[off], target(off))
            only(0)(lambda: send(stage, slot, buf.at[0], target(0)))

        def in_halves(kind, layer, picks, rhs, dims):
            def left(half):
                arrive(layer_stage(kind, layer, half))
                buf = slots[layer_stage(kind, layer, half)]
                return jnp.concatenate(
                    [jnp.concatenate([buf[idx] for idx in pick], axis=1) for pick in picks], axis=0)

            first = left(0)
            for off in DX:
                chosen[off] = mm(first, rhs(off, 0), dims)
            second = left(1)
            return lambda off: chosen[off] + mm(second, rhs(off, 1), dims)

        def item_columns(layer, prepare=None):
            def cols(off):
                return pl.ds(pl.multiple_of((yy + off) % 4 * 256, 256), 256)

            def rhs(off, half):
                return jnp.concatenate(
                    [adj[pl.ds(k * 256 + half * LANES, LANES), cols(off)] for k in range(4)], axis=0)

            def whole(off):
                prepare(cols(off))
                return mm(panel(EMB_USER), adj[:, cols(off)], NN)

            product = whole if prepare else in_halves(UAG, layer - 1, (range(4),), rhs, NN)
            spread_halves(IRS, layer, pos, part_item, DY, product, lambda off: at_y(off, 1))

        def user_products(layer):
            def rows(off):
                return pl.ds(pl.multiple_of((col + off) % 4 * 256, 256), 256)

            def rhs(off, half):
                return jnp.concatenate(
                    [adj[rows(off), pl.ds(k * 256 + half * LANES, LANES)] for k in range(4)], axis=1)

            def whole(off):
                return mm(panel(EMB_ITEM_B), adj[rows(off), :], NT)

            product = whole
            if layer > 1:
                product = in_halves(IAG, layer - 1, (range(4), range(4, 8)), rhs, NT)
            spread_halves(URS, layer, core * 4 + col, part_user, DX, product, lambda off: at_x(off, 1))

        @only(1)
        def _():
            arrive_one(DEG_ITEM_A)
            deg_sum = total(DEG_ITEM_A)
            small[2] = deg_sum
            slots[DEG_ITEM_B][zed] = deg_sum
            along_z(DEG_ITEM_B, small.at[2])

        arrive(EMB_ITEM_A)
        gathered = jnp.concatenate([slots[EMB_ITEM_A][k] for k in range(8)], axis=0)
        item_t = mm(eye(64, 64), gathered, NT).astype(BF16)
        item_tr[...] = item_t
        slots[EMB_ITEM_B][zed] = item_t
        for dz in DZ[:7]:
            send(EMB_ITEM_B, zed, item_tr, at_z(dz))
        arrive(DEG_USER)
        scale_user = lax.rsqrt(jnp.maximum(total(DEG_USER), 1.0))
        for k in range(8):
            su_col[pl.ds(k * LANES, LANES), :] = jnp.transpose(jnp.broadcast_to(scale_user[k:k + 1, :], (LANES, LANES)))

        def scale_rows(blk, carry):
            base = pl.multiple_of(blk * 32, 32)
            su = su_col[pl.ds(base, 32), :]
            for k in range(8):
                mask_su[pl.ds(base, 32), lanes(k)] = mask_v[pl.ds(base, 32), lanes(k)].astype(F32) * su
            return carry

        lax.fori_loop(0, 32, scale_rows, 0)
        lax.fori_loop(0, 64, one_hot, 0)
        arrive(EMB_USER)
        arrive(DEG_ITEM_B)
        scale_item = lax.rsqrt(jnp.maximum(total(DEG_ITEM_B), 1.0))
        for k in range(8):
            si_row[:, lanes(k)] = jnp.broadcast_to(scale_item[k:k + 1, :], (8, LANES))

        def prepare(cols):
            si = si_row[:, cols]

            def build(blk, carry):
                base = pl.multiple_of(blk * 128, 128)
                for k in range(8):
                    rows = pl.ds(pl.multiple_of(base + k * 16, 16), 16)
                    adj[rows, cols] = (mask_su[rows, cols] * jnp.concatenate([si, si], axis=0)).astype(BF16)
                return carry

            lax.fori_loop(0, 8, build, 0)

        def item_mid(layer, half):
            @only(1)
            def _():
                own = own_item.at[2 * (layer - 1) + half]
                stage = layer_stage(IRS, layer, half)
                arrive_one(stage)
                own[...] = total(stage)
                stage = layer_stage(IZZ, layer, half)
                for dz in DZ[:7]:
                    dims = pl.ds(pl.multiple_of((par + dz) % 2 * 32, 32), 32)
                    send(stage, zed, own.at[dims], at_z(dz))
                slots[stage][zed] = own[pl.ds(pl.multiple_of(par * 32, 32), 32)]

        def finish(val, tot, layer):
            tot[...] = tot[...] + val.astype(F32)
            return val if layer < LAYERS else (tot[...] * 0.25).astype(BF16)

        def user_end(layer, half):
            @only(1)
            def _():
                keep = user_src.at[2 * (layer - 1) + half]
                come = layer_stage(URS, layer, half)
                stage = layer_stage(UAG, layer, half)
                arrive_one(come)
                for which in (0, 1):
                    val = total(come, 4 * which, 4 * which + 4).astype(BF16)
                    res = finish(val, tot_user.at[which, half], layer)
                    keep[which] = res
                    for dx in DX:
                        if dx or not which:
                            send(stage, col, keep.at[which], at_x(dx, which))
                slots[stage][col] = res

        def item_end(layer, half):
            @only(1)
            def _():
                keep = out_half.at[2 * (layer - 1) + half]
                mine = par * 4 + yy
                come = layer_stage(IZZ, layer, half)
                stage = layer_stage(IAG, layer, half)
                arrive_one(come)
                res = finish(total(come).astype(BF16), tot_item.at[half], layer)
                keep[...] = res
                for which in (0, 1):
                    for plane in (zed - par + 1 - par, zed):
                        for dy in DY:
                            if plane is not zed or dy or not which:
                                send(stage, mine, keep, (col, plane * 8 + (yy + dy) % 4 * 2 + which))
                slots[stage][mine] = res

        item_columns(1, prepare)
        arrive(EMB_ITEM_B)
        user_products(1)

        @only(1)
        def _():
            arrive_one(EMB_MATE)
            dims = pl.ds(pl.multiple_of(par * 32, 32), 32)
            for half in (0, 1):
                tot_user[0, half] = slots[EMB_MATE][0, :, lanes(half)].astype(F32)
                tot_user[1, half] = user_t[:, lanes(half)].astype(F32)
                tot_item[half] = slots[EMB_ITEM_B][2 * yy + half, dims].astype(F32)

        for step in (item_mid, user_end):
            for half in (0, 1):
                step(1, half)
        for half in (0, 1):
            item_end(1, half)
        item_columns(2)
        user_products(2)
        for step in (item_mid, user_end, item_end):
            for half in (0, 1):
                step(2, half)
        item_columns(3)
        user_products(3)
        for half in (0, 1):
            item_mid(3, half)
        for step in (user_end, item_end):
            for half in (0, 1):
                step(3, half)
        arrive_both(UAG, 3)
        for half in (0, 1):
            out_user_ref[:, lanes(half)] = slots[layer_stage(UAG, 3, half)][col]
        out_panel = user_panel(3)
        for k in range(4):
            picked[k] = mm(out_panel, hot_user[:, k * 256:(k + 1) * 256], NN)
        def item_half(half):
            stage = layer_stage(IAG, LAYERS, half)
            arrive(stage)
            rows = [jnp.concatenate([slots[stage][k + idx] for idx in range(4)], axis=1) for k in (0, 4)]
            return jnp.concatenate(rows, axis=0)

        first = item_half(0)
        for k in range(4):
            chosen[k] = mm(first, hot_item[:512, k * 256:(k + 1) * 256], NN)
        second = item_half(1)
        for k in range(4):
            prod = (chosen[k] + mm(second, hot_item[512:, k * 256:(k + 1) * 256], NN)) * picked[k]
            red = jnp.sum(prod, axis=0, keepdims=True)
            for half in (0, 1):
                small[3, 2 * k + half:2 * k + half + 1, :] = red[:, lanes(half)]
        place = col * 8 + pos
        for dx in DX:
            for dy in DY:
                target = ((col + dx) % 4, zed * 8 + (yy + dy) % 4 * 2 + 1)
                if dx or dy:
                    send(LOSS_A, place, small.at[3], target)
                else:
                    only(0)(lambda: send(LOSS_A, place, small.at[3], target))

        @only(1)
        def _():
            slots[LOSS_A][place] = small[3]

        @only(1)
        def _():
            arrive_one(LOSS_A)
            val = total(LOSS_A)
            small[4] = val
            slots[LOSS_Z][zed] = val
            along_z(LOSS_Z, small.at[4])

        row_id = lax.broadcasted_iota(I32, (16, LANES), 0) + pos * 16
        col_id = lax.broadcasted_iota(I32, (16, LANES), 1)
        pick = jnp.where(row_id == col_id, 1.0, 0.0).astype(BF16)

        for half in (0, 1):
            @pl.when(par == half)
            def _():
                buf = slots[layer_stage(IAG, 3, half)]
                block = jnp.concatenate([buf[zed // 2], buf[4 + zed // 2]], axis=0)
                out_item_ref[...] = mm(pick, block, NT).astype(BF16)

        for which in (0, 1):
            @only(which)
            def _():
                for stage in range(len(STAGES)):
                    sent(stage, which)

        arrive(LOSS_Z)
        neg = -total(LOSS_Z)
        loss_ref[...] = jnp.maximum(neg, 0.0) + jnp.log1p(jnp.exp(-jnp.abs(neg)))

    body()


def hand_over(user_in, item_in, loss_in, user_out, item_out, loss_out, sems):
    pairs = ((user_in, user_out), (item_in, item_out), (loss_in, loss_out))
    copies = [pltpu.make_async_copy(src, dst, sems.at[k]) for k, (src, dst) in enumerate(pairs)]
    for cp in copies:
        cp.start()
    for cp in copies:
        cp.wait()


def solution(mesh):
    scratch = [pltpu.VMEM(*spec) for spec in SCRATCH]
    scratch += [pltpu.VMEM((stage[0],) + stage[1], stage[2]) for stage in STAGES]
    scratch += [pltpu.SemaphoreType.DMA((LOADS + 3,)), pltpu.SemaphoreType.DMA((len(STAGES),)),
                pltpu.SemaphoreType.DMA((len(STAGES),))]
    in_vmem = pl.BlockSpec(memory_space=pltpu.VMEM)
    outs = (jax.ShapeDtypeStruct((64, 256), BF16), jax.ShapeDtypeStruct((16, 64), BF16),
            jax.ShapeDtypeStruct((8, 128), F32))
    call = pl.pallas_call(
        functools.partial(kernel, tuple(mesh.axis_names)),
        out_shape=tuple(pltpu.VMEM(out.shape, out.dtype) for out in outs),
        in_specs=[pl.BlockSpec(memory_space=pl.ANY)] * 4,
        out_specs=(in_vmem, in_vmem, in_vmem),
        scratch_shapes=scratch,
        compiler_params=pltpu.CompilerParams(collective_id=0, has_side_effects=True),
    )
    pass_on = pl.pallas_call(
        hand_over, out_shape=outs, in_specs=[in_vmem] * 3,
        out_specs=(pl.BlockSpec(memory_space=pl.ANY),) * 3,
        scratch_shapes=[pltpu.SemaphoreType.DMA((3,))],
    )

    def device_body(mask_blk, user_shard, item_shard, triples):
        held = call(mask_blk, user_shard.T, item_shard, triples.T)
        out_user, out_item, loss = pass_on(*[pltpu.with_memory_space_constraint(x, pltpu.VMEM) for x in held])
        return out_user.T, out_item, loss.reshape(-1)

    return jax.shard_map(
        device_body,
        mesh=mesh,
        in_specs=(P("row", "col"), P(("row", "col"), None), P(("col", "row"), None), P()),
        out_specs=(P(("row", "col"), None), P(("col", "row"), None), P()),
        check_vma=False,
    )
```

```python
import functools

import jax
import jax.numpy as jnp
from jax import lax
from jax.experimental import pallas as pl
from jax.experimental.pallas import tpu as pltpu
from jax.sharding import PartitionSpec as P

LAYERS = 3
LANES = 128
LOADS = 16
F32 = jnp.float32
BF16 = jnp.bfloat16
I32 = jnp.int32
NT = (((1,), (1,)), ((), ()))
NN = (((1,), (0,)), ((), ()))

DX = (2, 1, 3, 0)
DY = (2, 1, 3, 0)
DZ = (4, 3, 5, 2, 6, 1, 7, 0)
EVERY = ((3, 3), (3, 3))
PLANE = ((7, 7), (7, 7))
GATHER = ((0, 7), (4, 3))
SPREAD = ((8, 7), (0, 15))
ROW = (8, LANES)
HALF = (64, LANES)
QUARTER = (32, LANES)
BLOCK = (64, 256)
STAGES = (
    (4, ROW, F32, *EVERY), (8, ROW, F32, *GATHER), (8, ROW, F32, *SPREAD),
    (4, BLOCK, BF16, *EVERY), (8, (16, 64), BF16, *PLANE), (8, HALF, BF16, *PLANE),
    (1, BLOCK, BF16, (0, 1), (1, 0)), (32, ROW, F32, (0, 31), (16, 15)), (8, ROW, F32, *SPREAD),
    *[(8, HALF, F32, *GATHER)] * 6,
    *[(4, HALF, BF16, (4, 3), (0, 7))] * 6,
    *[(8, HALF, F32, *GATHER)] * 6,
    *[(8, QUARTER, F32, (0, 7), (0, 7))] * 6,
    *[(8, QUARTER, BF16, *SPREAD)] * 6,
)
(DEG_USER, DEG_ITEM_A, DEG_ITEM_B, EMB_USER, EMB_ITEM_A, EMB_ITEM_B, EMB_MATE, LOSS_A, LOSS_Z) = range(9)
URS, UAG, IRS, IZZ, IAG = range(7, 37, 6)


def layer_stage(kind, layer, half):
    return kind + 2 * layer + half


SQUARE = (1024, 1024)
SCRATCH = (
    (SQUARE, I32), (SQUARE, F32), (SQUARE, BF16), (SQUARE, BF16), (SQUARE, BF16), ((1024, LANES), BF16),
    ((1024, LANES), F32), ((8, 1024), F32), ((3, 8, 1024), I32), ((5, *ROW), F32), (HALF, BF16),
    ((6, 2, *HALF), BF16), ((6, 4, *HALF), F32), ((6, 4, *HALF), F32), ((6, *HALF), F32), ((6, *QUARTER), BF16),
    (BLOCK, BF16), ((16, 64), BF16), ((3, 1024), I32), ((4, *BLOCK), F32), ((4, *BLOCK), F32),
    ((2, 2, *HALF), F32), ((2, *QUARTER), F32),
)


def mm(lhs, rhs, dims):
    return lax.dot_general(lhs, rhs, dims, preferred_element_type=F32)


def eye(rows, cols):
    row_id = lax.broadcasted_iota(I32, (rows, cols), 0)
    col_id = lax.broadcasted_iota(I32, (rows, cols), 1)
    return jnp.where(row_id == col_id, 1.0, 0.0).astype(BF16)


def kernel(axis_names, mask_hbm, user_hbm, item_hbm, trip_hbm, out_user_ref, out_item_ref, loss_ref, *refs):
    (mask_v, mask_su, adj, hot_user, hot_item, row_part, su_col, si_row, ids, small, item_tr, user_src,
     part_user, part_item, own_item, out_half, user_ref, item_ref, trip_ref, picked, chosen,
     tot_user, tot_item) = refs[:len(SCRATCH)]
    slots = refs[len(SCRATCH):-3]
    load_sem, send_sem, recv_sem = refs[-3:]
    row = lax.axis_index("row")
    col = lax.axis_index("col")
    zed = row // 8
    pos = row % 8
    yy = pos // 2
    core = pos % 2
    par = zed % 2
    loads = []

    def only(which):
        return pl.when(core == which)

    def device(to_col, to_row):
        return tuple(to_col if name == "col" else to_row for name in axis_names)

    def at_x(dx, which=None):
        return (col + dx) % 4, row if which is None else row - core + which

    def at_y(dy, which):
        return col, zed * 8 + (yy + dy) % 4 * 2 + which

    def at_z(dz, which=None):
        return col, (zed + dz) % 8 * 8 + (pos if which is None else yy * 2 + which)

    def send(stage, slot, src, target):
        pltpu.make_async_remote_copy(
            src_ref=src, dst_ref=slots[stage].at[slot],
            send_sem=send_sem.at[stage], recv_sem=recv_sem.at[stage],
            device_id=device(*target), device_id_type=pl.DeviceIdType.MESH).start()

    def batch(stage, count):
        part = slots[stage].at[pl.ds(0, count)]
        return pltpu.make_async_remote_copy(
            src_ref=part, dst_ref=part, send_sem=send_sem.at[stage], recv_sem=recv_sem.at[stage],
            device_id=device(*at_x(1)), device_id_type=pl.DeviceIdType.MESH)

    def arrive(stage):
        count = STAGES[stage][3]
        if count[0] == count[1]:
            batch(stage, count[0]).wait_recv()
        else:
            for which in (0, 1):
                if count[which]:
                    only(which)(batch(stage, count[which]).wait_recv)

    def arrive_one(stage):
        batch(stage, STAGES[stage][3][1]).wait_recv()

    def sent(stage, which):
        left = STAGES[stage][4][which]
        while left:
            count = min(left, STAGES[stage][0])
            batch(stage, count).wait_send()
            left -= count

    def total(stage, first=0, last=None):
        buf = slots[stage]
        acc = buf[first]
        for idx in range(first + 1, last or STAGES[stage][0]):
            acc = acc + buf[idx]
        return acc

    def panel(stage):
        buf = slots[stage]
        return jnp.concatenate([buf[idx] for idx in range(STAGES[stage][0])], axis=1)

    def columns(kind, layer, picks):
        bufs = [slots[layer_stage(kind, layer, half)] for half in (0, 1)]
        return jnp.concatenate([buf[idx] for idx in picks for buf in bufs], axis=1)

    def user_panel(layer):
        return columns(UAG, layer, range(4))

    def arrive_both(kind, layer):
        for half in (0, 1):
            arrive(layer_stage(kind, layer, half))

    def lanes(k):
        return slice(k * LANES, (k + 1) * LANES)

    def load(src, dst):
        cp = pltpu.make_async_copy(src, dst, load_sem.at[len(loads)])
        cp.start()
        loads.append(cp)
        return cp

    def to_owners(stage, slot, src, local):
        for dy in DY[:3]:
            send(stage, slot, src, at_y(dy, 1))
        only(0)(lambda: send(stage, slot, src, at_y(0, 1)))

        @only(1)
        def _():
            slots[stage][slot] = local

    def along_z(stage, src):
        for dz in DZ:
            for which in (0, 1):
                if dz or not which:
                    send(stage, zed, src, at_z(dz, which))

    def body():
        for q in range(LOADS):
            rows = pl.ds(q * (1024 // LOADS), 1024 // LOADS)
            load(mask_hbm.at[rows], mask_v.at[rows])
        user_cp = load(user_hbm, user_ref)
        item_cp = load(item_hbm, item_ref)
        trip_cp = load(trip_hbm, trip_ref)
        barrier = pltpu.get_barrier_semaphore()
        targets = [at_z(dz, which) for dz in DZ[:7] for which in (0, 1)]
        targets += [((col + dx) % 4, zed * 8 + (pos + off) % 8) for dx in DX for off in range(8) if dx or off]
        targets += [(col, (zed - par + 1 - par) * 8 + (yy + dy) % 4 * 2 + which) for dy in DY[:3] for which in (0, 1)]
        for target in targets:
            pl.semaphore_signal(barrier, inc=1, device_id=device(*target), device_id_type=pl.DeviceIdType.MESH)
        n_peers = len(targets)


        def degree_rows(blk, acc):
            base = pl.multiple_of(blk * 32, 32)
            m = mask_v[pl.ds(base, 32), :].astype(F32)
            part = m[:, lanes(0)]
            for k in range(1, 8):
                part = part + m[:, lanes(k)]
            row_part[pl.ds(base, 32), :] = part.astype(BF16)
            return acc + ((m[0:8] + m[8:16]) + (m[16:24] + m[24:32]))

        acc = jnp.zeros((8, 1024), F32)
        trips = 32 // LOADS
        for q in range(LOADS):
            loads[q].wait()
            acc = lax.fori_loop(q * trips, (q + 1) * trips, degree_rows, acc)
        col_sum = jnp.sum(acc, axis=0, keepdims=True)
        for k in range(8):
            small[0, k:k + 1, :] = col_sum[:, lanes(k)]
        row_sum = mm(jnp.ones((8, LANES), BF16), row_part[...], NT)
        for k in range(8):
            small[1, k:k + 1, :] = row_sum[0:1, lanes(k)]
        slots[DEG_USER][col] = small[1]
        for cp in (user_cp, item_cp, trip_cp):
            cp.wait()
        pl.semaphore_wait(barrier, n_peers)
        to_owners(DEG_ITEM_A, pos, small.at[0], small[0])
        for dx in DX[:3]:
            send(DEG_USER, col, small.at[1], at_x(dx))
        for dx in DX[:3]:
            send(EMB_USER, col, user_ref, at_x(dx))
        for off in (4, 5, 3, 2, 6, 7, 1):
            send(EMB_ITEM_A, pos, item_ref, (col, zed * 8 + (pos + off) % 8))
        only(0)(lambda: send(EMB_MATE, 0, user_ref, at_y(0, 1)))
        user_t = user_ref[...]
        slots[EMB_USER][col] = user_t
        slots[EMB_ITEM_A][pos] = item_ref[...]
        for k, block in enumerate((row, col, col)):
            ids[k] = jnp.broadcast_to(trip_ref[k:k + 1, :] - block * 1024, (8, 1024))

        def one_hot(blk, carry):
            base = pl.multiple_of(blk * 16, 16)
            base_item = base // 512 * LANES + base % 512 // LANES * 256 + base % LANES
            for k in range(8):
                hits = []
                for half in range(2):
                    sub = lax.broadcasted_iota(I32, ROW, 0) + half * 8
                    near = (sub + base, sub + base_item, sub + base_item)
                    hits.append([jnp.where(ids[w, :, lanes(k)] == near[w], 1.0, 0.0) for w in range(3)])
                hot_user[pl.ds(base, 16), lanes(k)] = jnp.concatenate([hit[0] for hit in hits], axis=0).astype(BF16)
                hot_item[pl.ds(base, 16), lanes(k)] = jnp.concatenate([hit[1] - hit[2] for hit in hits], axis=0).astype(BF16)
            return carry

        def spread_halves(kind, layer, slot, store, offsets, product, target):
            for off in offsets:
                res = product(off)
                for half in (0, 1):
                    buf = store.at[2 * (layer - 1) + half]
                    if off:
                        buf[off] = res[:, lanes(half)]
                        if not half:
                            send(layer_stage(kind, layer, half), slot, buf.at[off], target(off))
                    else:
                        @only(0)
                        def _():
                            buf[off] = res[:, lanes(half)]
                            if not half:
                                send(layer_stage(kind, layer, half), slot, buf.at[off], target(off))

                        @only(1)
                        def _():
                            slots[layer_stage(kind, layer, half)][slot] = res[:, lanes(half)]
            stage = layer_stage(kind, layer, 1)
            buf = store.at[2 * layer - 1]
            for off in offsets[:3]:
                send(stage, slot, buf.at[off], target(off))
            only(0)(lambda: send(stage, slot, buf.at[0], target(0)))

        def in_halves(kind, layer, picks, rhs, dims):
            def left(half):
                arrive(layer_stage(kind, layer, half))
                buf = slots[layer_stage(kind, layer, half)]
                return jnp.concatenate(
                    [jnp.concatenate([buf[idx] for idx in pick], axis=1) for pick in picks], axis=0)

            first = left(0)
            for off in DX:
                chosen[off] = mm(first, rhs(off, 0), dims)
            second = left(1)
            return lambda off: chosen[off] + mm(second, rhs(off, 1), dims)

        def item_columns(layer, prepare=None):
            def cols(off):
                return pl.ds(pl.multiple_of((yy + off) % 4 * 256, 256), 256)

            def rhs(off, half):
                return jnp.concatenate(
                    [adj[pl.ds(k * 256 + half * LANES, LANES), cols(off)] for k in range(4)], axis=0)

            def whole(off):
                prepare(cols(off))
                return mm(panel(EMB_USER), adj[:, cols(off)], NN)

            product = whole if prepare else in_halves(UAG, layer - 1, (range(4),), rhs, NN)
            spread_halves(IRS, layer, pos, part_item, DY, product, lambda off: at_y(off, 1))

        def user_products(layer):
            def rows(off):
                return pl.ds(pl.multiple_of((col + off) % 4 * 256, 256), 256)

            def rhs(off, half):
                return jnp.concatenate(
                    [adj[rows(off), pl.ds(k * 256 + half * LANES, LANES)] for k in range(4)], axis=1)

            def whole(off):
                return mm(panel(EMB_ITEM_B), adj[rows(off), :], NT)

            product = whole
            if layer > 1:
                product = in_halves(IAG, layer - 1, (range(4), range(4, 8)), rhs, NT)
            spread_halves(URS, layer, core * 4 + col, part_user, DX, product, lambda off: at_x(off, 1))

        @only(1)
        def _():
            arrive_one(DEG_ITEM_A)
            deg_sum = total(DEG_ITEM_A)
            small[2] = deg_sum
            slots[DEG_ITEM_B][zed] = deg_sum
            along_z(DEG_ITEM_B, small.at[2])

        arrive(EMB_ITEM_A)
        gathered = jnp.concatenate([slots[EMB_ITEM_A][k] for k in range(8)], axis=0)
        item_t = mm(eye(64, 64), gathered, NT).astype(BF16)
        item_tr[...] = item_t
        slots[EMB_ITEM_B][zed] = item_t
        for dz in DZ[:7]:
            send(EMB_ITEM_B, zed, item_tr, at_z(dz))
        arrive(DEG_USER)
        scale_user = lax.rsqrt(jnp.maximum(total(DEG_USER), 1.0))
        for k in range(8):
            su_col[pl.ds(k * LANES, LANES), :] = jnp.transpose(jnp.broadcast_to(scale_user[k:k + 1, :], (LANES, LANES)))

        def scale_rows(blk, carry):
            base = pl.multiple_of(blk * 32, 32)
            su = su_col[pl.ds(base, 32), :]
            for k in range(8):
                mask_su[pl.ds(base, 32), lanes(k)] = mask_v[pl.ds(base, 32), lanes(k)].astype(F32) * su
            return carry

        lax.fori_loop(0, 32, scale_rows, 0)
        lax.fori_loop(0, 64, one_hot, 0)
        arrive(EMB_USER)
        arrive(DEG_ITEM_B)
        scale_item = lax.rsqrt(jnp.maximum(total(DEG_ITEM_B), 1.0))
        for k in range(8):
            si_row[:, lanes(k)] = jnp.broadcast_to(scale_item[k:k + 1, :], (8, LANES))

        def prepare(cols):
            si = si_row[:, cols]

            def build(blk, carry):
                base = pl.multiple_of(blk * 128, 128)
                for k in range(8):
                    rows = pl.ds(pl.multiple_of(base + k * 16, 16), 16)
                    adj[rows, cols] = (mask_su[rows, cols] * jnp.concatenate([si, si], axis=0)).astype(BF16)
                return carry

            lax.fori_loop(0, 8, build, 0)

        def item_mid(layer, half):
            @only(1)
            def _():
                own = own_item.at[2 * (layer - 1) + half]
                stage = layer_stage(IRS, layer, half)
                arrive_one(stage)
                own[...] = total(stage)
                stage = layer_stage(IZZ, layer, half)
                for dz in DZ[:7]:
                    dims = pl.ds(pl.multiple_of((par + dz) % 2 * 32, 32), 32)
                    send(stage, zed, own.at[dims], at_z(dz))
                slots[stage][zed] = own[pl.ds(pl.multiple_of(par * 32, 32), 32)]

        def finish(val, tot, layer):
            tot[...] = tot[...] + val.astype(F32)
            return val if layer < LAYERS else (tot[...] * 0.25).astype(BF16)

        def user_end(layer, half):
            @only(1)
            def _():
                keep = user_src.at[2 * (layer - 1) + half]
                come = layer_stage(URS, layer, half)
                stage = layer_stage(UAG, layer, half)
                arrive_one(come)
                for which in (0, 1):
                    val = total(come, 4 * which, 4 * which + 4).astype(BF16)
                    res = finish(val, tot_user.at[which, half], layer)
                    keep[which] = res
                    for dx in DX:
                        if dx or not which:
                            send(stage, col, keep.at[which], at_x(dx, which))
                slots[stage][col] = res

        def item_end(layer, half):
            @only(1)
            def _():
                keep = out_half.at[2 * (layer - 1) + half]
                mine = par * 4 + yy
                come = layer_stage(IZZ, layer, half)
                stage = layer_stage(IAG, layer, half)
                arrive_one(come)
                res = finish(total(come).astype(BF16), tot_item.at[half], layer)
                keep[...] = res
                for which in (0, 1):
                    for plane in (zed - par + 1 - par, zed):
                        for dy in DY:
                            if plane is not zed or dy or not which:
                                send(stage, mine, keep, (col, plane * 8 + (yy + dy) % 4 * 2 + which))
                slots[stage][mine] = res

        item_columns(1, prepare)
        arrive(EMB_ITEM_B)
        user_products(1)

        @only(1)
        def _():
            arrive_one(EMB_MATE)
            dims = pl.ds(pl.multiple_of(par * 32, 32), 32)
            for half in (0, 1):
                tot_user[0, half] = slots[EMB_MATE][0, :, lanes(half)].astype(F32)
                tot_user[1, half] = user_t[:, lanes(half)].astype(F32)
                tot_item[half] = slots[EMB_ITEM_B][2 * yy + half, dims].astype(F32)

        for step in (item_mid, user_end):
            for half in (0, 1):
                step(1, half)
        for half in (0, 1):
            item_end(1, half)
        item_columns(2)
        user_products(2)
        for step in (item_mid, user_end, item_end):
            for half in (0, 1):
                step(2, half)
        item_columns(3)
        user_products(3)
        for half in (0, 1):
            item_mid(3, half)
        for step in (user_end, item_end):
            for half in (0, 1):
                step(3, half)
        arrive_both(UAG, 3)
        for half in (0, 1):
            out_user_ref[:, lanes(half)] = slots[layer_stage(UAG, 3, half)][col]
        out_panel = user_panel(3)
        for k in range(4):
            picked[k] = mm(out_panel, hot_user[:, k * 256:(k + 1) * 256], NN)
        def item_half(half):
            stage = layer_stage(IAG, LAYERS, half)
            arrive(stage)
            rows = [jnp.concatenate([slots[stage][k + idx] for idx in range(4)], axis=1) for k in (0, 4)]
            return jnp.concatenate(rows, axis=0)

        first = item_half(0)
        for k in range(4):
            chosen[k] = mm(first, hot_item[:512, k * 256:(k + 1) * 256], NN)
        second = item_half(1)
        for k in range(4):
            prod = (chosen[k] + mm(second, hot_item[512:, k * 256:(k + 1) * 256], NN)) * picked[k]
            red = jnp.sum(prod, axis=0, keepdims=True)
            for half in (0, 1):
                small[3, 2 * k + half:2 * k + half + 1, :] = red[:, lanes(half)]
        place = col * 8 + pos
        for dx in DX:
            for dy in DY:
                target = ((col + dx) % 4, zed * 8 + (yy + dy) % 4 * 2 + 1)
                if dx or dy:
                    send(LOSS_A, place, small.at[3], target)
                else:
                    only(0)(lambda: send(LOSS_A, place, small.at[3], target))

        @only(1)
        def _():
            slots[LOSS_A][place] = small[3]

        @only(1)
        def _():
            arrive_one(LOSS_A)
            val = total(LOSS_A)
            small[4] = val
            slots[LOSS_Z][zed] = val
            along_z(LOSS_Z, small.at[4])

        row_id = lax.broadcasted_iota(I32, (16, LANES), 0) + pos * 16
        col_id = lax.broadcasted_iota(I32, (16, LANES), 1)
        pick = jnp.where(row_id == col_id, 1.0, 0.0).astype(BF16)

        for half in (0, 1):
            @pl.when(par == half)
            def _():
                buf = slots[layer_stage(IAG, 3, half)]
                block = jnp.concatenate([buf[zed // 2], buf[4 + zed // 2]], axis=0)
                out_item_ref[...] = mm(pick, block, NT).astype(BF16)

        for which in (0, 1):
            @only(which)
            def _():
                for stage in range(len(STAGES)):
                    sent(stage, which)

        arrive(LOSS_Z)
        neg = -total(LOSS_Z)
        loss_ref[...] = jnp.maximum(neg, 0.0) + jnp.log1p(jnp.exp(-jnp.abs(neg)))

    body()


def hand_over(user_in, item_in, loss_in, user_out, item_out, loss_out, sems):
    pairs = ((user_in, user_out), (item_in, item_out), (loss_in, loss_out))
    copies = [pltpu.make_async_copy(src, dst, sems.at[k]) for k, (src, dst) in enumerate(pairs)]
    for cp in copies:
        cp.start()
    for cp in copies:
        cp.wait()


def solution(mesh):
    scratch = [pltpu.VMEM(*spec) for spec in SCRATCH]
    scratch += [pltpu.VMEM((stage[0],) + stage[1], stage[2]) for stage in STAGES]
    scratch += [pltpu.SemaphoreType.DMA((LOADS + 3,)), pltpu.SemaphoreType.DMA((len(STAGES),)),
                pltpu.SemaphoreType.DMA((len(STAGES),))]
    in_vmem = pl.BlockSpec(memory_space=pltpu.VMEM)
    outs = (jax.ShapeDtypeStruct((64, 256), BF16), jax.ShapeDtypeStruct((16, 64), BF16),
            jax.ShapeDtypeStruct((8, 128), F32))
    call = pl.pallas_call(
        functools.partial(kernel, tuple(mesh.axis_names)),
        out_shape=tuple(pltpu.VMEM(out.shape, out.dtype) for out in outs),
        in_specs=[pl.BlockSpec(memory_space=pl.ANY)] * 4,
        out_specs=(in_vmem, in_vmem, in_vmem),
        scratch_shapes=scratch,
        compiler_params=pltpu.CompilerParams(collective_id=0, has_side_effects=True),
    )
    pass_on = pl.pallas_call(
        hand_over, out_shape=outs, in_specs=[in_vmem] * 3,
        out_specs=(pl.BlockSpec(memory_space=pl.ANY),) * 3,
        scratch_shapes=[pltpu.SemaphoreType.DMA((3,))],
    )

    def device_body(mask_blk, user_shard, item_shard, triples):
        held = call(mask_blk, user_shard.T, item_shard, triples.T)
        out_user, out_item, loss = pass_on(*[pltpu.with_memory_space_constraint(x, pltpu.VMEM) for x in held])
        return out_user.T, out_item, loss.reshape(-1)

    return jax.shard_map(
        device_body,
        mesh=mesh,
        in_specs=(P("row", "col"), P(("row", "col"), None), P(("col", "row"), None), P()),
        out_specs=(P(("row", "col"), None), P(("col", "row"), None), P()),
        check_vma=False,
    )
```

```python
import functools

import jax
import jax.numpy as jnp
from jax import lax
from jax.experimental import pallas as pl
from jax.experimental.pallas import tpu as pltpu
from jax.sharding import PartitionSpec as P

LAYERS = 3
LANES = 128
LOADS = 16
F32 = jnp.float32
BF16 = jnp.bfloat16
I32 = jnp.int32
NT = (((1,), (1,)), ((), ()))
NN = (((1,), (0,)), ((), ()))

DX = (2, 1, 3, 0)
DY = (2, 1, 3, 0)
DZ = (4, 3, 5, 2, 6, 1, 7, 0)
EVERY = ((3, 3), (3, 3))
PLANE = ((7, 7), (7, 7))
GATHER = ((0, 7), (4, 3))
SPREAD = ((8, 7), (0, 15))
ROW = (8, LANES)
HALF = (64, LANES)
QUARTER = (32, LANES)
BLOCK = (64, 256)
STAGES = (
    (4, ROW, F32, *EVERY), (8, ROW, F32, *GATHER), (8, ROW, F32, *SPREAD),
    (4, BLOCK, BF16, *EVERY), (8, (16, 64), BF16, *PLANE), (8, HALF, BF16, *PLANE),
    (1, BLOCK, BF16, (0, 1), (1, 0)), (32, ROW, F32, (0, 31), (16, 15)), (8, ROW, F32, *SPREAD),
    *[(8, HALF, F32, *GATHER)] * 6,
    *[(4, HALF, BF16, (4, 3), (0, 7))] * 6,
    *[(8, HALF, F32, *GATHER)] * 6,
    *[(8, QUARTER, F32, (0, 7), (0, 7))] * 6,
    *[(8, QUARTER, BF16, *SPREAD)] * 6,
)
(DEG_USER, DEG_ITEM_A, DEG_ITEM_B, EMB_USER, EMB_ITEM_A, EMB_ITEM_B, EMB_MATE, LOSS_A, LOSS_Z) = range(9)
URS, UAG, IRS, IZZ, IAG = range(7, 37, 6)


def layer_stage(kind, layer, half):
    return kind + 2 * layer + half


SQUARE = (1024, 1024)
SCRATCH = (
    (SQUARE, I32), (SQUARE, F32), (SQUARE, BF16), (SQUARE, BF16), (SQUARE, BF16), ((1024, LANES), BF16),
    ((1024, LANES), F32), ((8, 1024), F32), ((3, 8, 1024), I32), ((5, *ROW), F32), (HALF, BF16),
    ((6, 2, *HALF), BF16), ((6, 4, *HALF), F32), ((6, 4, *HALF), F32), ((6, *HALF), F32), ((6, *QUARTER), BF16),
    (BLOCK, BF16), ((16, 64), BF16), ((3, 1024), I32), ((4, *BLOCK), F32), ((4, *BLOCK), F32),
    ((2, 2, *HALF), F32), ((2, *QUARTER), F32),
)


def mm(lhs, rhs, dims):
    return lax.dot_general(lhs, rhs, dims, preferred_element_type=F32)


def eye(rows, cols):
    row_id = lax.broadcasted_iota(I32, (rows, cols), 0)
    col_id = lax.broadcasted_iota(I32, (rows, cols), 1)
    return jnp.where(row_id == col_id, 1.0, 0.0).astype(BF16)


def kernel(axis_names, mask_hbm, user_hbm, item_hbm, trip_hbm, out_user_ref, out_item_ref, loss_ref, *refs):
    (mask_v, mask_su, adj, hot_user, hot_item, row_part, su_col, si_row, ids, small, item_tr, user_src,
     part_user, part_item, own_item, out_half, user_ref, item_ref, trip_ref, picked, chosen,
     tot_user, tot_item) = refs[:len(SCRATCH)]
    slots = refs[len(SCRATCH):-3]
    load_sem, send_sem, recv_sem = refs[-3:]
    row = lax.axis_index("row")
    col = lax.axis_index("col")
    zed = row // 8
    pos = row % 8
    yy = pos // 2
    core = pos % 2
    par = zed % 2
    loads = []

    def only(which):
        return pl.when(core == which)

    def device(to_col, to_row):
        return tuple(to_col if name == "col" else to_row for name in axis_names)

    def at_x(dx, which=None):
        return (col + dx) % 4, row if which is None else row - core + which

    def at_y(dy, which):
        return col, zed * 8 + (yy + dy) % 4 * 2 + which

    def at_z(dz, which=None):
        return col, (zed + dz) % 8 * 8 + (pos if which is None else yy * 2 + which)

    def send(stage, slot, src, target):
        pltpu.make_async_remote_copy(
            src_ref=src, dst_ref=slots[stage].at[slot],
            send_sem=send_sem.at[stage], recv_sem=recv_sem.at[stage],
            device_id=device(*target), device_id_type=pl.DeviceIdType.MESH).start()

    def batch(stage, count):
        part = slots[stage].at[pl.ds(0, count)]
        return pltpu.make_async_remote_copy(
            src_ref=part, dst_ref=part, send_sem=send_sem.at[stage], recv_sem=recv_sem.at[stage],
            device_id=device(*at_x(1)), device_id_type=pl.DeviceIdType.MESH)

    def arrive(stage):
        count = STAGES[stage][3]
        if count[0] == count[1]:
            batch(stage, count[0]).wait_recv()
        else:
            for which in (0, 1):
                if count[which]:
                    only(which)(batch(stage, count[which]).wait_recv)

    def arrive_one(stage):
        batch(stage, STAGES[stage][3][1]).wait_recv()

    def sent(stage, which):
        left = STAGES[stage][4][which]
        while left:
            count = min(left, STAGES[stage][0])
            batch(stage, count).wait_send()
            left -= count

    def total(stage, first=0, last=None):
        buf = slots[stage]
        acc = buf[first]
        for idx in range(first + 1, last or STAGES[stage][0]):
            acc = acc + buf[idx]
        return acc

    def panel(stage):
        buf = slots[stage]
        return jnp.concatenate([buf[idx] for idx in range(STAGES[stage][0])], axis=1)

    def columns(kind, layer, picks):
        bufs = [slots[layer_stage(kind, layer, half)] for half in (0, 1)]
        return jnp.concatenate([buf[idx] for idx in picks for buf in bufs], axis=1)

    def user_panel(layer):
        return columns(UAG, layer, range(4))

    def arrive_both(kind, layer):
        for half in (0, 1):
            arrive(layer_stage(kind, layer, half))

    def lanes(k):
        return slice(k * LANES, (k + 1) * LANES)

    def load(src, dst):
        cp = pltpu.make_async_copy(src, dst, load_sem.at[len(loads)])
        cp.start()
        loads.append(cp)
        return cp

    def to_owners(stage, slot, src, local):
        for dy in DY[:3]:
            send(stage, slot, src, at_y(dy, 1))
        only(0)(lambda: send(stage, slot, src, at_y(0, 1)))

        @only(1)
        def _():
            slots[stage][slot] = local

    def along_z(stage, src):
        for dz in DZ:
            for which in (0, 1):
                if dz or not which:
                    send(stage, zed, src, at_z(dz, which))

    def body():
        for q in range(LOADS):
            rows = pl.ds(q * (1024 // LOADS), 1024 // LOADS)
            load(mask_hbm.at[rows], mask_v.at[rows])
        user_cp = load(user_hbm, user_ref)
        item_cp = load(item_hbm, item_ref)
        trip_cp = load(trip_hbm, trip_ref)
        barrier = pltpu.get_barrier_semaphore()
        targets = [at_z(dz, which) for dz in DZ[:7] for which in (0, 1)]
        targets += [((col + dx) % 4, zed * 8 + (pos + off) % 8) for dx in DX for off in range(8) if dx or off]
        targets += [(col, (zed - par + 1 - par) * 8 + (yy + dy) % 4 * 2 + which) for dy in DY[:3] for which in (0, 1)]
        for target in targets:
            pl.semaphore_signal(barrier, inc=1, device_id=device(*target), device_id_type=pl.DeviceIdType.MESH)
        n_peers = len(targets)


        def degree_rows(blk, acc):
            base = pl.multiple_of(blk * 32, 32)
            m = mask_v[pl.ds(base, 32), :].astype(F32)
            part = m[:, lanes(0)]
            for k in range(1, 8):
                part = part + m[:, lanes(k)]
            row_part[pl.ds(base, 32), :] = part.astype(BF16)
            return acc + ((m[0:8] + m[8:16]) + (m[16:24] + m[24:32]))

        acc = jnp.zeros((8, 1024), F32)
        trips = 32 // LOADS
        for q in range(LOADS):
            loads[q].wait()
            acc = lax.fori_loop(q * trips, (q + 1) * trips, degree_rows, acc)
        col_sum = jnp.sum(acc, axis=0, keepdims=True)
        for k in range(8):
            small[0, k:k + 1, :] = col_sum[:, lanes(k)]
        row_sum = mm(jnp.ones((8, LANES), BF16), row_part[...], NT)
        for k in range(8):
            small[1, k:k + 1, :] = row_sum[0:1, lanes(k)]
        slots[DEG_USER][col] = small[1]
        for cp in (user_cp, item_cp, trip_cp):
            cp.wait()
        pl.semaphore_wait(barrier, n_peers)
        to_owners(DEG_ITEM_A, pos, small.at[0], small[0])
        for dx in DX[:3]:
            send(DEG_USER, col, small.at[1], at_x(dx))
        for dx in DX[:3]:
            send(EMB_USER, col, user_ref, at_x(dx))
        for off in (4, 5, 3, 2, 6, 7, 1):
            send(EMB_ITEM_A, pos, item_ref, (col, zed * 8 + (pos + off) % 8))
        only(0)(lambda: send(EMB_MATE, 0, user_ref, at_y(0, 1)))
        user_t = user_ref[...]
        slots[EMB_USER][col] = user_t
        slots[EMB_ITEM_A][pos] = item_ref[...]
        for k, block in enumerate((row, col, col)):
            ids[k] = jnp.broadcast_to(trip_ref[k:k + 1, :] - block * 1024, (8, 1024))

        def one_hot(blk, carry):
            base = pl.multiple_of(blk * 16, 16)
            base_item = base // 512 * LANES + base % 512 // LANES * 256 + base % LANES
            for k in range(8):
                hits = []
                for half in range(2):
                    sub = lax.broadcasted_iota(I32, ROW, 0) + half * 8
                    near = (sub + base, sub + base_item, sub + base_item)
                    hits.append([jnp.where(ids[w, :, lanes(k)] == near[w], 1.0, 0.0) for w in range(3)])
                hot_user[pl.ds(base, 16), lanes(k)] = jnp.concatenate([hit[0] for hit in hits], axis=0).astype(BF16)
                hot_item[pl.ds(base, 16), lanes(k)] = jnp.concatenate([hit[1] - hit[2] for hit in hits], axis=0).astype(BF16)
            return carry

        def spread_halves(kind, layer, slot, store, offsets, product, target):
            for off in offsets:
                res = product(off)
                for half in (0, 1):
                    buf = store.at[2 * (layer - 1) + half]
                    if off:
                        buf[off] = res[:, lanes(half)]
                        if not half:
                            send(layer_stage(kind, layer, half), slot, buf.at[off], target(off))
                    else:
                        @only(0)
                        def _():
                            buf[off] = res[:, lanes(half)]
                            if not half:
                                send(layer_stage(kind, layer, half), slot, buf.at[off], target(off))

                        @only(1)
                        def _():
                            slots[layer_stage(kind, layer, half)][slot] = res[:, lanes(half)]
            stage = layer_stage(kind, layer, 1)
            buf = store.at[2 * layer - 1]
            for off in offsets[:3]:
                send(stage, slot, buf.at[off], target(off))
            only(0)(lambda: send(stage, slot, buf.at[0], target(0)))

        def in_halves(kind, layer, picks, rhs, dims):
            def left(half):
                arrive(layer_stage(kind, layer, half))
                buf = slots[layer_stage(kind, layer, half)]
                return jnp.concatenate(
                    [jnp.concatenate([buf[idx] for idx in pick], axis=1) for pick in picks], axis=0)

            first = left(0)
            for off in DX:
                chosen[off] = mm(first, rhs(off, 0), dims)
            second = left(1)
            return lambda off: chosen[off] + mm(second, rhs(off, 1), dims)

        def item_columns(layer, prepare=None):
            def cols(off):
                return pl.ds(pl.multiple_of((yy + off) % 4 * 256, 256), 256)

            def rhs(off, half):
                return jnp.concatenate(
                    [adj[pl.ds(k * 256 + half * LANES, LANES), cols(off)] for k in range(4)], axis=0)

            def whole(off):
                prepare(cols(off))
                return mm(panel(EMB_USER), adj[:, cols(off)], NN)

            product = whole if prepare else in_halves(UAG, layer - 1, (range(4),), rhs, NN)
            spread_halves(IRS, layer, pos, part_item, DY, product, lambda off: at_y(off, 1))

        def user_products(layer):
            def rows(off):
                return pl.ds(pl.multiple_of((col + off) % 4 * 256, 256), 256)

            def rhs(off, half):
                return jnp.concatenate(
                    [adj[rows(off), pl.ds(k * 256 + half * LANES, LANES)] for k in range(4)], axis=1)

            def whole(off):
                return mm(panel(EMB_ITEM_B), adj[rows(off), :], NT)

            product = whole
            if layer > 1:
                product = in_halves(IAG, layer - 1, (range(4), range(4, 8)), rhs, NT)
            spread_halves(URS, layer, core * 4 + col, part_user, DX, product, lambda off: at_x(off, 1))

        @only(1)
        def _():
            arrive_one(DEG_ITEM_A)
            deg_sum = total(DEG_ITEM_A)
            small[2] = deg_sum
            slots[DEG_ITEM_B][zed] = deg_sum
            along_z(DEG_ITEM_B, small.at[2])

        arrive(EMB_ITEM_A)
        gathered = jnp.concatenate([slots[EMB_ITEM_A][k] for k in range(8)], axis=0)
        item_t = mm(eye(64, 64), gathered, NT).astype(BF16)
        item_tr[...] = item_t
        slots[EMB_ITEM_B][zed] = item_t
        for dz in DZ[:7]:
            send(EMB_ITEM_B, zed, item_tr, at_z(dz))
        arrive(DEG_USER)
        scale_user = lax.rsqrt(jnp.maximum(total(DEG_USER), 1.0))
        for k in range(8):
            su_col[pl.ds(k * LANES, LANES), :] = jnp.transpose(jnp.broadcast_to(scale_user[k:k + 1, :], (LANES, LANES)))

        def scale_rows(blk, carry):
            base = pl.multiple_of(blk * 32, 32)
            su = su_col[pl.ds(base, 32), :]
            for k in range(8):
                mask_su[pl.ds(base, 32), lanes(k)] = mask_v[pl.ds(base, 32), lanes(k)].astype(F32) * su
            return carry

        lax.fori_loop(0, 32, scale_rows, 0)
        lax.fori_loop(0, 64, one_hot, 0)
        arrive(EMB_USER)
        arrive(DEG_ITEM_B)
        scale_item = lax.rsqrt(jnp.maximum(total(DEG_ITEM_B), 1.0))
        for k in range(8):
            si_row[:, lanes(k)] = jnp.broadcast_to(scale_item[k:k + 1, :], (8, LANES))

        def prepare(cols):
            si = si_row[:, cols]

            si2 = jnp.concatenate([si, si], axis=0)
            for k in range(64):
                rows = slice(k * 16, (k + 1) * 16)
                adj[rows, cols] = (mask_su[rows, cols] * si2).astype(BF16)

        def item_mid(layer, half):
            @only(1)
            def _():
                own = own_item.at[2 * (layer - 1) + half]
                stage = layer_stage(IRS, layer, half)
                arrive_one(stage)
                own[...] = total(stage)
                stage = layer_stage(IZZ, layer, half)
                for dz in DZ[:7]:
                    dims = pl.ds(pl.multiple_of((par + dz) % 2 * 32, 32), 32)
                    send(stage, zed, own.at[dims], at_z(dz))
                slots[stage][zed] = own[pl.ds(pl.multiple_of(par * 32, 32), 32)]

        def finish(val, tot, layer):
            tot[...] = tot[...] + val.astype(F32)
            return val if layer < LAYERS else (tot[...] * 0.25).astype(BF16)

        def user_end(layer, half):
            @only(1)
            def _():
                keep = user_src.at[2 * (layer - 1) + half]
                come = layer_stage(URS, layer, half)
                stage = layer_stage(UAG, layer, half)
                arrive_one(come)
                for which in (0, 1):
                    val = total(come, 4 * which, 4 * which + 4).astype(BF16)
                    res = finish(val, tot_user.at[which, half], layer)
                    keep[which] = res
                    for dx in DX:
                        if dx or not which:
                            send(stage, col, keep.at[which], at_x(dx, which))
                slots[stage][col] = res

        def item_end(layer, half):
            @only(1)
            def _():
                keep = out_half.at[2 * (layer - 1) + half]
                mine = par * 4 + yy
                come = layer_stage(IZZ, layer, half)
                stage = layer_stage(IAG, layer, half)
                arrive_one(come)
                res = finish(total(come).astype(BF16), tot_item.at[half], layer)
                keep[...] = res
                for which in (0, 1):
                    for plane in (zed - par + 1 - par, zed):
                        for dy in DY:
                            if plane is not zed or dy or not which:
                                send(stage, mine, keep, (col, plane * 8 + (yy + dy) % 4 * 2 + which))
                slots[stage][mine] = res

        item_columns(1, prepare)
        arrive(EMB_ITEM_B)
        user_products(1)

        @only(1)
        def _():
            arrive_one(EMB_MATE)
            dims = pl.ds(pl.multiple_of(par * 32, 32), 32)
            for half in (0, 1):
                tot_user[0, half] = slots[EMB_MATE][0, :, lanes(half)].astype(F32)
                tot_user[1, half] = user_t[:, lanes(half)].astype(F32)
                tot_item[half] = slots[EMB_ITEM_B][2 * yy + half, dims].astype(F32)

        for step in (item_mid, user_end):
            for half in (0, 1):
                step(1, half)
        for half in (0, 1):
            item_end(1, half)
        item_columns(2)
        user_products(2)
        for step in (item_mid, user_end, item_end):
            for half in (0, 1):
                step(2, half)
        item_columns(3)
        user_products(3)
        for half in (0, 1):
            item_mid(3, half)
        for step in (user_end, item_end):
            for half in (0, 1):
                step(3, half)
        arrive_both(UAG, 3)
        for half in (0, 1):
            out_user_ref[:, lanes(half)] = slots[layer_stage(UAG, 3, half)][col]
        out_panel = user_panel(3)
        for k in range(4):
            picked[k] = mm(out_panel, hot_user[:, k * 256:(k + 1) * 256], NN)
        def item_half(half):
            stage = layer_stage(IAG, LAYERS, half)
            arrive(stage)
            rows = [jnp.concatenate([slots[stage][k + idx] for idx in range(4)], axis=1) for k in (0, 4)]
            return jnp.concatenate(rows, axis=0)

        first = item_half(0)
        for k in range(4):
            chosen[k] = mm(first, hot_item[:512, k * 256:(k + 1) * 256], NN)
        second = item_half(1)
        for k in range(4):
            prod = (chosen[k] + mm(second, hot_item[512:, k * 256:(k + 1) * 256], NN)) * picked[k]
            red = jnp.sum(prod, axis=0, keepdims=True)
            for half in (0, 1):
                small[3, 2 * k + half:2 * k + half + 1, :] = red[:, lanes(half)]
        place = col * 8 + pos
        for dx in DX:
            for dy in DY:
                target = ((col + dx) % 4, zed * 8 + (yy + dy) % 4 * 2 + 1)
                if dx or dy:
                    send(LOSS_A, place, small.at[3], target)
                else:
                    only(0)(lambda: send(LOSS_A, place, small.at[3], target))

        @only(1)
        def _():
            slots[LOSS_A][place] = small[3]

        @only(1)
        def _():
            arrive_one(LOSS_A)
            val = total(LOSS_A)
            small[4] = val
            slots[LOSS_Z][zed] = val
            along_z(LOSS_Z, small.at[4])

        row_id = lax.broadcasted_iota(I32, (16, LANES), 0) + pos * 16
        col_id = lax.broadcasted_iota(I32, (16, LANES), 1)
        pick = jnp.where(row_id == col_id, 1.0, 0.0).astype(BF16)

        for half in (0, 1):
            @pl.when(par == half)
            def _():
                buf = slots[layer_stage(IAG, 3, half)]
                block = jnp.concatenate([buf[zed // 2], buf[4 + zed // 2]], axis=0)
                out_item_ref[...] = mm(pick, block, NT).astype(BF16)

        for which in (0, 1):
            @only(which)
            def _():
                for stage in range(len(STAGES)):
                    sent(stage, which)

        arrive(LOSS_Z)
        neg = -total(LOSS_Z)
        loss_ref[...] = jnp.maximum(neg, 0.0) + jnp.log1p(jnp.exp(-jnp.abs(neg)))

    body()


def hand_over(user_in, item_in, loss_in, user_out, item_out, loss_out, sems):
    pairs = ((user_in, user_out), (item_in, item_out), (loss_in, loss_out))
    copies = [pltpu.make_async_copy(src, dst, sems.at[k]) for k, (src, dst) in enumerate(pairs)]
    for cp in copies:
        cp.start()
    for cp in copies:
        cp.wait()


def solution(mesh):
    scratch = [pltpu.VMEM(*spec) for spec in SCRATCH]
    scratch += [pltpu.VMEM((stage[0],) + stage[1], stage[2]) for stage in STAGES]
    scratch += [pltpu.SemaphoreType.DMA((LOADS + 3,)), pltpu.SemaphoreType.DMA((len(STAGES),)),
                pltpu.SemaphoreType.DMA((len(STAGES),))]
    in_vmem = pl.BlockSpec(memory_space=pltpu.VMEM)
    outs = (jax.ShapeDtypeStruct((64, 256), BF16), jax.ShapeDtypeStruct((16, 64), BF16),
            jax.ShapeDtypeStruct((8, 128), F32))
    call = pl.pallas_call(
        functools.partial(kernel, tuple(mesh.axis_names)),
        out_shape=tuple(pltpu.VMEM(out.shape, out.dtype) for out in outs),
        in_specs=[pl.BlockSpec(memory_space=pl.ANY)] * 4,
        out_specs=(in_vmem, in_vmem, in_vmem),
        scratch_shapes=scratch,
        compiler_params=pltpu.CompilerParams(collective_id=0, has_side_effects=True),
    )
    pass_on = pl.pallas_call(
        hand_over, out_shape=outs, in_specs=[in_vmem] * 3,
        out_specs=(pl.BlockSpec(memory_space=pl.ANY),) * 3,
        scratch_shapes=[pltpu.SemaphoreType.DMA((3,))],
    )

    def device_body(mask_blk, user_shard, item_shard, triples):
        held = call(mask_blk, user_shard.T, item_shard, triples.T)
        out_user, out_item, loss = pass_on(*[pltpu.with_memory_space_constraint(x, pltpu.VMEM) for x in held])
        return out_user.T, out_item, loss.reshape(-1)

    return jax.shard_map(
        device_body,
        mesh=mesh,
        in_specs=(P("row", "col"), P(("row", "col"), None), P(("col", "row"), None), P()),
        out_specs=(P(("row", "col"), None), P(("col", "row"), None), P()),
        check_vma=False,
    )
```
